512 devices in a mesh: bytes: 16 (over z), ctx: 8 (over x, core), tp: 4 (over y).
Axes of the slice: x: 4, y: 4, z: 16, core: 2. Of those that a mesh axis runs over, the one named last changes fastest.
Arguments:
- byte_values_sequence: int32 [24576], P(('bytes', 'ctx')), may hold values from 0 to 255
- offsets: int32 [24576], P(('bytes', 'ctx')), may hold values from 0 to 168, as said below
- byte_table: bfloat16 [256, 1024], replicated, may hold values from -6 to 6
- byte_query: bfloat16 [1024, 1024], P(None, 'tp'), may hold values from -1 to 1
- byte_key: bfloat16 [1024, 1024], P(None, 'tp'), may hold values from -16 to 16
- byte_value: bfloat16 [1024, 1024], P(None, 'tp'), may hold values from -0.1875 to 0.1875
- latent_query: bfloat16 [1024, 4096], P(None, ('ctx', 'tp')), may hold values from -1 to 1
- latent_key: bfloat16 [1024, 4096], P(None, ('ctx', 'tp')), may hold values from -16 to 16
- latent_value: bfloat16 [1024, 4096], P(None, ('ctx', 'tp')), may hold values from -0.1875 to 0.1875
- decode_weight: bfloat16 [4096, 1024], P(('ctx', 'tp')), may hold values from -1 to 1
Outputs:
- byte_output: bfloat16 [24576, 1024], P(('bytes', 'ctx'), 'tp')
The draws below stay inside these ranges and needn't reach their ends.
Inputs may be any that keep to these rules, and one draw needn't show every extreme that they name: offsets[i] is 0 where a patch starts and offsets[i - 1] + 1 elsewhere; the first byte of every device's 192 bytes starts a patch; one device's bytes hold 24 to 72 patch starts and the bytes of the devices of one index of bytes hold at most 384; both most values are reached in every draw.
All inputs are finite; a program needn't handle non-finite values.
Results may differ from the reference program's by a relative error of at most 0.017.
Values may be sent and summed in bfloat16 or wider, within the bound.
No kernel may reach another device: no remote copies, remote signals or barrier semaphores. Data moves between devices by JAX's collectives and lax.ppermute only.
A program may use at most 64 MiB of HBM per device.

```python
import math
import jax
import jax.numpy as jnp
import numpy as np
from jax import lax

BYTES_DEV = 192
DB = 1024
HEADS_B = 16
HEADS_L = 32
HEAD_L = 128
VOCAB = 256
BLOCKS = 128
SEQ = 24576
PCAP = 72
GCAP = 384
PATCHES = 6144


def draw_offsets(key, part):
    per_group = GCAP * 4 // BYTES_DEV
    groups = BLOCKS // per_group
    lowest = BYTES_DEV // 8
    headroom = PCAP - lowest
    budget = GCAP - per_group * lowest
    key_surplus, key_group, key_places = jax.random.split(key, 3)
    key_sparse = jax.random.fold_in(key, 29)
    surplus = jax.random.randint(key_surplus, (groups, per_group), 0, headroom + 1, dtype=jnp.int32)
    forced = jax.random.randint(key_group, (), 0, groups, dtype=jnp.int32)
    sparse_group = jax.random.randint(key_sparse, (), 0, groups, dtype=jnp.int32)
    surplus = jnp.where((jnp.arange(groups, dtype=jnp.int32) == forced)[:, None], headroom, surplus)
    sparse_cell = (jnp.arange(groups, dtype=jnp.int32) == sparse_group)[:, None] & (jnp.arange(per_group, dtype=jnp.int32) == per_group - 1)[None, :]
    surplus = jnp.where(sparse_cell, 0, surplus)
    capped = jnp.minimum(jnp.cumsum(surplus, axis=1), budget)
    surplus = capped - jnp.concatenate([jnp.zeros((groups, 1), jnp.int32), capped[:, :-1]], axis=1)
    counts = (lowest + surplus).reshape(BLOCKS)
    places = jnp.arange(BYTES_DEV, dtype=jnp.int32)
    attention_scores = jax.random.randint(key_places, (BLOCKS, BYTES_DEV), 1, 1 << 20, dtype=jnp.int32) * BYTES_DEV + places[None, :]
    sparse_block = sparse_group * per_group + per_group - 1
    is_sparse = (jnp.arange(BLOCKS, dtype=jnp.int32) == sparse_block)[:, None]
    tail_scores = jnp.where(places >= BYTES_DEV - lowest + 1, places, (1 << 20) * BYTES_DEV + places)
    attention_scores = jnp.where(is_sparse, tail_scores[None, :], attention_scores)
    attention_scores = jnp.where(places[None, :] == 0, 0, attention_scores)
    ranking = jnp.argsort(jnp.argsort(attention_scores, axis=1, stable=True), axis=1, stable=True)
    starts = (ranking < counts[:, None]).reshape(SEQ)
    indices = jnp.arange(SEQ, dtype=jnp.int32)
    latest = lax.cummax(jnp.where(starts, indices, 0), axis=0)
    return (indices - latest).astype(jnp.int32)


def paired(key, salt_value, fan_in, head_count, head_feature_width):
    query_key_product, key_other = jax.random.split(jax.random.fold_in(key, salt_value), 2)
    dimensions = (fan_in, head_count * head_feature_width)
    queries = jnp.clip(jax.random.normal(query_key_product, dimensions, jnp.float32) * fan_in ** (-0.5), -1.0, 1.0)
    key_side = jax.random.normal(key_other, dimensions, jnp.float32) * fan_in ** (-0.5)
    return (queries, jnp.clip(key_side, -16.0, 16.0))


def draw_byte_query(key, part):
    return paired(key, 11, DB, HEADS_B, DB // HEADS_B)[0].astype(jnp.bfloat16)


def draw_byte_key(key, part):
    return paired(key, 11, DB, HEADS_B, DB // HEADS_B)[1].astype(jnp.bfloat16)


def draw_latent_query(key, part):
    return paired(key, 13, DB, HEADS_L, HEAD_L)[0].astype(jnp.bfloat16)


def draw_latent_key(key, part):
    return paired(key, 13, DB, HEADS_L, HEAD_L)[1].astype(jnp.bfloat16)


def touch_ends(values, stream_key, least, largest):
    dims = values.shape
    place = [jax.random.randint(jax.random.fold_in(stream_key, axis), (), 0, dims[axis]) for axis in range(len(dims))]
    values = values.at[tuple(place)].set(least)
    longest = dims.index(max(dims))
    place[longest] = (place[longest] + 1) % dims[longest]
    return values.at[tuple(place)].set(largest)


def spiked(result, rng, source, target, blocks, factor):
    def block_of(axis_at):
        return (jnp.arange(result.shape[axis_at]) // (result.shape[axis_at] // blocks)).reshape((-1,) + (1,) * (result.ndim - 1 - axis_at))

    first = jax.random.permutation(rng, blocks)[block_of(target)]
    second = (block_of(target) + blocks // 2) % blocks
    return jnp.where((block_of(source) == first) | (block_of(source) == second), factor * result, result)


def block_levels(stream_key, shape, shards, least, high):
    factor_of, own = 1.0, jax.random.fold_in(stream_key, 6)
    for dim, blocks in shards:
        steps = jnp.exp(jax.random.uniform(jax.random.fold_in(own, dim), (blocks,), jnp.float32, least / len(shards), high / len(shards)))
        factor_of = factor_of * jnp.repeat(steps, shape[dim] // blocks).reshape([-1 if axis == dim else 1 for axis in range(len(shape))])
    return factor_of


def rank_bounds(count, skew):
    portions = [(1 << 20) // math.isqrt(grade ** skew) + 1 for grade in range(1, count + 1)]
    scale = 1 + sum(portions) // (1 << 30)
    return np.cumsum(np.array([max(1, weight // scale) for weight in portions]))


def skewed_ids(stream_key, extent, amount, slope):
    listing = rank_bounds(amount, slope)
    ticket = jax.random.randint(jax.random.fold_in(stream_key, 1), extent, 0, int(listing[amount - 1]))
    standing = jnp.searchsorted(jnp.asarray(listing, jnp.int32), ticket, side="right")
    return jax.random.permutation(jax.random.fold_in(stream_key, 2), amount)[standing].astype(jnp.int32)


def noise(stream_key, shape, scale, bound, shards=(), held_as=jnp.bfloat16):
    gain = block_levels(stream_key, shape, shards, -0.22, 0.18) if shards else 1.0
    drawn = jax.random.normal(stream_key, shape, jnp.float32) * scale * gain
    return jnp.minimum(jnp.maximum(drawn, -bound), bound).astype(held_as)


def bell_draw_with(stream_key, shape, scale, most, cuts, heavy, kind=jnp.bfloat16):
    drawn = scale * jax.random.normal(stream_key, shape, jnp.float32)
    if cuts:
        drawn = drawn * block_levels(stream_key, shape, cuts, -0.22, 0.18)
    return jnp.clip(spiked(drawn, jax.random.fold_in(stream_key, 3), *heavy), -most, most).astype(kind)


def setup_inputs(seed: int = 0) -> dict:
    streams_of = jax.random.split(jax.random.key(seed), 11)
    return {
        "byte_values_sequence": touch_ends(skewed_ids(streams_of[0], (SEQ,), VOCAB, 2), jax.random.fold_in(streams_of[0], 3), 0, VOCAB - 1).astype(jnp.int32),
        "offsets": draw_offsets(jax.random.fold_in(streams_of[10], 71), 0),
        "byte_table": noise(streams_of[2], (VOCAB, DB), 1.0, 6.0),
        "byte_query": draw_byte_query(jax.random.fold_in(streams_of[10], 71), 0),
        "byte_key": draw_byte_key(jax.random.fold_in(streams_of[10], 71), 0),
        "byte_value": noise(streams_of[5], (DB, DB), DB ** -0.5, 0.1875, ((1, 4),)),
        "latent_query": draw_latent_query(jax.random.fold_in(streams_of[10], 71), 0),
        "latent_key": draw_latent_key(jax.random.fold_in(streams_of[10], 71), 0),
        "latent_value": noise(streams_of[8], (DB, HEADS_L * HEAD_L), DB ** -0.5, 0.1875, ((1, 32),)),
        "decode_weight": bell_draw_with(streams_of[9], (HEADS_L * HEAD_L, DB), HEAD_L ** -0.5, 1.0, ((0, 32),), (0, 1, 32, 2.75)),
    }


EPSILON = 1e-06
NEGATIVE = -1e+30

def norm_rows(values):
    values = values.astype(jnp.float32)
    return values * lax.rsqrt(lax.optimization_barrier(jnp.mean(values * values, axis=-1, keepdims=True)) + EPSILON)

def rounded(values):
    return lax.optimization_barrier(values.astype(jnp.bfloat16)).astype(jnp.float32)

def project(inputs, weight):
    return jnp.dot(inputs, weight, preferred_element_type=jnp.float32).astype(jnp.bfloat16)

def softmax_mix(attention_scores, allowed, values):
    attention_scores = jnp.where(allowed, attention_scores, NEGATIVE)
    highest = lax.optimization_barrier(jnp.max(attention_scores, axis=-1, keepdims=True))
    weights = jnp.where(allowed, jnp.exp(attention_scores - highest), 0.0)
    totals = lax.optimization_barrier(jnp.sum(weights, axis=-1, keepdims=True))
    blended = jnp.einsum('...qk,...kd->...qd', rounded(weights), values, precision=lax.Precision.HIGHEST)
    return blended / totals

def reference(byte_values_sequence, offsets, byte_table, byte_query, byte_key, byte_value, latent_query, latent_key, latent_value, decode_weight):
    head_feature_width = DB // HEADS_B
    block_count = SEQ // BYTES_DEV
    normed = norm_rows(byte_table[byte_values_sequence]).astype(jnp.bfloat16)
    byte_window_queries = project(normed, byte_query)
    byte_window_keys = project(normed, byte_key)
    values_b = project(normed, byte_value)
    query_pos = jnp.arange(BYTES_DEV, dtype=jnp.int32)[:, None]
    key_pos = jnp.arange(2 * BYTES_DEV, dtype=jnp.int32)[None, :]
    inside = (key_pos > query_pos) & (key_pos <= query_pos + BYTES_DEV)
    opening = (jnp.arange(block_count, dtype=jnp.int32) == 0)[:, None, None] & (key_pos < BYTES_DEV)[None]
    allowed_b = inside[None] & jnp.logical_not(opening)

    def keys_with_earlier(blocks):
        earlier = jnp.concatenate([jnp.zeros_like(blocks[:1]), blocks[:-1]], axis=0)
        return jnp.concatenate([earlier, blocks], axis=1)

    def byte_head(head_index):

        def column_positions(values):
            picked = lax.dynamic_slice_in_dim(values, head_index * head_feature_width, head_feature_width, 1)
            return picked.astype(jnp.float32).reshape(block_count, BYTES_DEV, head_feature_width)
        attention_scores = jnp.einsum('gye,gje->gyj', column_positions(byte_window_queries), keys_with_earlier(column_positions(byte_window_keys)), precision=lax.Precision.HIGHEST) / math.sqrt(head_feature_width)
        blended = softmax_mix(attention_scores, allowed_b, keys_with_earlier(column_positions(values_b)))
        return blended.reshape(SEQ, head_feature_width)
    encoded = lax.map(byte_head, jnp.arange(HEADS_B, dtype=jnp.int32))
    encoded = encoded.transpose(1, 0, 2).reshape(SEQ, DB).astype(jnp.bfloat16)
    patch_of = jnp.cumsum((offsets == 0).astype(jnp.int32)) - 1
    lengths = jax.ops.segment_sum(jnp.ones((SEQ,), jnp.float32), patch_of, num_segments=PATCHES)
    patch_sums = jax.ops.segment_sum(encoded.astype(jnp.float32), patch_of, num_segments=PATCHES)
    pooled = (patch_sums / jnp.maximum(lengths, 1.0)[:, None]).astype(jnp.bfloat16)
    latent_in = norm_rows(pooled).astype(jnp.bfloat16)
    patch_ids = jnp.arange(PATCHES, dtype=jnp.int32)
    present = patch_ids <= patch_of[-1]
    queries_l = project(latent_in, latent_query)
    keys_l = project(latent_in, latent_key)
    values_l = project(latent_in, latent_value)
    block_rows = math.gcd(PATCHES, 512)

    def latent_head(head_index):

        def column_positions(values):
            return lax.dynamic_slice_in_dim(values, head_index * HEAD_L, HEAD_L, 1).astype(jnp.float32)
        queries_h = column_positions(queries_l)
        keys_h = column_positions(keys_l)
        values_h = column_positions(values_l)

        def query_block(block_index):
            picked = lax.dynamic_slice_in_dim(queries_h, block_index * block_rows, block_rows, 0)
            ordinals = block_index * block_rows + jnp.arange(block_rows, dtype=jnp.int32)
            allowed = (patch_ids[None, :] <= ordinals[:, None]) & present[None, :]
            attention_scores = jnp.dot(picked, keys_h.T, precision=lax.Precision.HIGHEST) / math.sqrt(HEAD_L)
            return softmax_mix(attention_scores, allowed, values_h)
        blended = lax.map(query_block, jnp.arange(PATCHES // block_rows, dtype=jnp.int32))
        return blended.reshape(PATCHES, HEAD_L)
    latent_out = lax.map(latent_head, jnp.arange(HEADS_L, dtype=jnp.int32))
    latent_out = latent_out.transpose(1, 0, 2).reshape(PATCHES, HEADS_L * HEAD_L).astype(jnp.bfloat16)
    decoded = jnp.dot(latent_out, decode_weight, preferred_element_type=jnp.float32)
    return (encoded.astype(jnp.float32) + decoded[patch_of]).astype(jnp.bfloat16)
```

```python
import math

import jax
import jax.numpy as jnp
from jax import lax
from jax.experimental import pallas as pl
from jax.experimental.pallas import tpu as pltpu
from jax.sharding import PartitionSpec as P

DB = 1024
HEADS_B = 16
HEAD_L = 128
SLOTS = 72
ROWS = 80
GROUP = 384
KVROWS = 400
EPSILON = 1e-06
NEGATIVE = -1e30
F32 = jnp.float32
BF16 = jnp.bfloat16


VMEM = pl.BlockSpec(memory_space=pltpu.VMEM)
SMEM = pl.BlockSpec(memory_space=pltpu.SMEM)


def iota(shape, dim):
    return lax.broadcasted_iota(jnp.int32, shape, dim)


def dot(a, b):
    return jnp.dot(a, b, preferred_element_type=F32)


def dot_nt(a, b):
    return lax.dot_general(a, b, (((1,), (1,)), ((), ())), preferred_element_type=F32)


def dot_tn(a, b):
    return lax.dot_general(a, b, (((0,), (0,)), ((), ())), preferred_element_type=F32)


def table_kernel(table_ref, wq_ref, wk_ref, wv_ref, out_ref):
    embedded = table_ref[...].astype(F32)
    scale = lax.rsqrt(jnp.mean(embedded * embedded, axis=-1, keepdims=True) + EPSILON)
    normed = (embedded * scale).astype(BF16)
    for k, w_ref in enumerate((wq_ref, wk_ref, wv_ref)):
        out_ref[:, 256 * k : 256 * (k + 1)] = dot(normed, w_ref[...]).astype(BF16)


def byte_kernel(block_ref, ids_ref, earlier_ref, offsets_ref, table_ref, enc_ref, member_ref, pay_ref):
    n = ids_ref.shape[1]
    vocab = table_ref.shape[0]
    width = enc_ref.shape[1]
    onehot = (iota((vocab, n), 0) == ids_ref[...]).astype(F32).astype(BF16)
    onehot_e = (iota((vocab, n), 0) == earlier_ref[...]).astype(F32).astype(BF16)
    own = dot_tn(onehot, table_ref[...]).astype(BF16)
    before = dot_tn(onehot_e, table_ref[:, width:]).astype(BF16)
    queries = own[:, :width]
    keys = jnp.concatenate([before[:, :width], own[:, width : 2 * width]], axis=0)
    values = jnp.concatenate([before[:, width:], own[:, 2 * width :]], axis=0)
    query_pos = iota((n, 2 * n), 0)
    key_pos = iota((n, 2 * n), 1)
    first = jnp.where(block_ref[0] > 0, 0, n)
    allowed = (key_pos > query_pos) & (key_pos <= query_pos + n) & (key_pos >= first)
    head = 64
    encoded = jnp.zeros((n, width), F32)
    for h in range(width // head):
        column = iota((1, width), 1)
        mine = ((column >= h * head) & (column < (h + 1) * head)).astype(F32).astype(BF16)
        scores = dot_nt(queries * mine, keys) * (1.0 / math.sqrt(head))
        scores = jnp.where(allowed, scores, NEGATIVE)
        weights = jnp.exp(scores - jnp.max(scores, axis=-1, keepdims=True))
        totals = jnp.sum(weights, axis=-1, keepdims=True)
        encoded = encoded + dot(weights.astype(BF16), values * mine) / totals
    encoded = encoded.astype(BF16)
    enc_ref[...] = encoded
    starts = (offsets_ref[...] == 0).astype(F32)
    upto = (iota((n, n), 0) <= iota((n, n), 1)).astype(F32).astype(BF16)
    running = dot(jnp.broadcast_to(starts, (8, n)).astype(BF16), upto)[0:1]
    patch = running.astype(jnp.int32) - 1
    members = (iota((ROWS, n), 0) == patch).astype(F32)
    member_ref[...] = members.astype(BF16)
    lengths = jnp.sum(members, axis=1, keepdims=True)
    pooled = dot(members.astype(BF16), encoded) / jnp.maximum(lengths, 1.0)
    count = jnp.sum(starts, axis=1, keepdims=True)
    payload = jnp.where(iota((ROWS, width), 0) == SLOTS, count, pooled).astype(BF16)
    for i in range(pay_ref.shape[0]):
        pay_ref[i] = payload


def latent_kernel(got_ref, wq_ref, wk_ref, wv_ref, q_ref, kv_ref, place_ref):
    blocks = got_ref.shape[0] // 4
    slot = iota((1, ROWS * blocks), 1)
    count = jnp.zeros((1, ROWS * blocks), F32)
    ahead = jnp.zeros((1, ROWS * blocks), F32)
    total = jnp.zeros((1, 1), F32)
    for c in range(blocks):
        here = got_ref[4 * c][SLOTS : SLOTS + 1, 0:1].astype(F32)
        inside = (slot >= ROWS * c) & (slot < ROWS * (c + 1))
        count = jnp.where(inside, here, count)
        ahead = jnp.where(inside, total - float(ROWS * c), ahead)
        total = total + here
    index = slot.astype(F32)
    position = index + ahead
    start = jnp.zeros_like(index)
    for c in range(1, blocks):
        start = jnp.where(slot >= ROWS * c, float(ROWS * c), start)
    place = jnp.where(index - start < count, position, -1.0).astype(jnp.int32)
    place_ref[...] = jnp.broadcast_to(place, place_ref.shape)
    queries, keys, values = [], [], []
    for c in range(blocks):
        parts = [got_ref[4 * c + t].astype(F32) for t in range(4)]
        square = sum(jnp.sum(p * p, axis=-1, keepdims=True) for p in parts)
        scale = lax.rsqrt(square * (1.0 / DB) + EPSILON)
        latent = jnp.concatenate([(p * scale).astype(BF16) for p in parts], axis=1)
        queries.append(dot(latent, wq_ref[...]).astype(BF16))
        keys.append(dot(latent, wk_ref[...]).astype(BF16))
        values.append(dot(latent, wv_ref[...]).astype(BF16))
    pick = (iota((GROUP, ROWS * blocks), 0) == place).astype(F32).astype(BF16)
    q_ref[...] = dot(pick, jnp.concatenate(queries, axis=0)).astype(BF16)
    kv_ref[0:GROUP, 0:HEAD_L] = dot(pick, jnp.concatenate(keys, axis=0)).astype(BF16)
    kv_ref[0:GROUP, HEAD_L:] = dot(pick, jnp.concatenate(values, axis=0)).astype(BF16)
    high = total.astype(BF16).astype(F32)
    row = iota((KVROWS - GROUP, 2 * HEAD_L), 0)
    tail = jnp.where(row == 0, high, jnp.where(row == 1, total - high, 0.0))
    kv_ref[GROUP:, :] = tail.astype(BF16)


SCALE = 1.0 / math.sqrt(HEAD_L)


def own_kernel(q_ref, kv_ref, m_ref, l_ref, acc_ref):
    scores = dot_nt(q_ref[...], kv_ref[0:GROUP, 0:HEAD_L]) * SCALE
    scores = jnp.where(iota((GROUP, GROUP), 1) <= iota((GROUP, GROUP), 0), scores, NEGATIVE)
    highest = jnp.max(scores, axis=-1, keepdims=True)
    weights = jnp.exp(scores - highest)
    m_ref[...] = jnp.broadcast_to(highest, m_ref.shape)
    l_ref[...] = jnp.broadcast_to(jnp.sum(weights, axis=-1, keepdims=True), l_ref.shape)
    acc_ref[...] = dot(weights.astype(BF16), kv_ref[0:GROUP, HEAD_L:])


def make_step(step, size, two):
    def step_kernel(z_ref, q_ref, *refs):
        kv_refs = refs[: 1 + two]
        m_in, l_in, acc_in, m_ref, l_ref, acc_ref = refs[1 + two :]
        m_ref[...] = m_in[...]
        l_ref[...] = l_in[...]
        acc_ref[...] = acc_in[...]
        z = z_ref[0]
        for kv_ref, valid in zip(kv_refs, (z >= step, z + step >= size)):

            @pl.when(valid)
            def _(kv_ref=kv_ref):
                filled = (kv_ref[GROUP : GROUP + 1, 0:1].astype(F32) + kv_ref[GROUP + 1 : GROUP + 2, 0:1].astype(F32))
                scores = dot_nt(q_ref[...], kv_ref[0:GROUP, 0:HEAD_L]) * SCALE
                present = iota((1, GROUP), 1).astype(F32) < filled
                scores = jnp.where(present, scores, NEGATIVE)
                old = m_ref[:, 0:1]
                highest = jnp.maximum(old, jnp.max(scores, axis=-1, keepdims=True))
                factor = jnp.exp(old - highest)
                weights = jnp.exp(scores - highest)
                m_ref[...] = jnp.broadcast_to(highest, m_ref.shape)
                l_ref[...] = l_ref[...] * factor + jnp.sum(weights, axis=-1, keepdims=True)
                acc_ref[...] = acc_ref[...] * factor + dot(weights.astype(BF16), kv_ref[0:GROUP, HEAD_L:])

    return step_kernel


def share_kernel(l_ref, acc_ref, place_ref, w_ref, out_ref):
    out = (acc_ref[...] / l_ref[...]).astype(BF16)
    slots = place_ref.shape[1]
    pick = (iota((GROUP, slots), 0) == place_ref[0:1]).astype(F32).astype(BF16)
    spread = dot_tn(pick, out).astype(BF16)
    width = out_ref.shape[2]
    for t in range(4):
        part = dot(spread, w_ref[:, width * t : width * (t + 1)]).astype(BF16)
        for c in range(slots // ROWS):
            out_ref[4 * c + t] = part[ROWS * c : ROWS * c + SLOTS]


def output_kernel(got_ref, enc_ref, member_ref, out_ref):
    decoded = got_ref[0].astype(F32)
    for h in range(1, got_ref.shape[0]):
        decoded = decoded + got_ref[h].astype(F32)
    decoded = jnp.concatenate([decoded, jnp.zeros((ROWS - SLOTS, decoded.shape[1]), F32)], axis=0)
    high = decoded.astype(BF16)
    low = (decoded - high.astype(F32)).astype(BF16)
    members = member_ref[...]
    out_ref[...] = (enc_ref[...].astype(F32) + dot_tn(members, high) + dot_tn(members, low)).astype(BF16)


def call(kernel, shapes, specs, *args):
    single = not isinstance(shapes, list)
    structs = [jax.ShapeDtypeStruct(s, d) for s, d in ([shapes] if single else shapes)]
    return pl.pallas_call(
        kernel,
        out_shape=structs[0] if single else structs,
        in_specs=specs,
        out_specs=VMEM if single else [VMEM] * len(structs),
    )(*args)


def shift(value, steps):
    size = lax.axis_size("bytes")
    return lax.ppermute(value, "bytes", [(i, (i + steps) % size) for i in range(size)])


def per_device(ids, offsets, byte_table, byte_query, byte_key, byte_value, latent_query, latent_key, latent_value, decode_weight):
    n = ids.shape[0]
    width = byte_query.shape[1]
    size = lax.axis_size("bytes")
    plane = lax.axis_size(("ctx", "tp"))
    z = lax.axis_index("bytes").astype(jnp.int32).reshape(1)
    block = lax.axis_index(("bytes", "ctx")).astype(jnp.int32).reshape(1)
    count = lax.axis_size(("bytes", "ctx"))
    earlier = lax.ppermute(ids, ("bytes", "ctx"), [(i, i + 1) for i in range(count - 1)])
    table = call(table_kernel, ((byte_table.shape[0], 3 * width), BF16), [VMEM] * 4, byte_table, byte_query, byte_key, byte_value)
    encoded, members, payload = call(
        byte_kernel,
        [((n, width), BF16), ((ROWS, n), BF16), ((plane, ROWS, width), BF16)],
        [SMEM] + [VMEM] * 4,
        block, ids.reshape(1, n), earlier.reshape(1, n), offsets.reshape(1, n), table,
    )
    got = lax.all_to_all(payload, ("ctx", "tp"), split_axis=0, concat_axis=0, tiled=True)
    queries, kv, place = call(
        latent_kernel,
        [((GROUP, HEAD_L), BF16), ((KVROWS, 2 * HEAD_L), BF16), ((8, ROWS * plane // 4), jnp.int32)],
        [VMEM] * 4,
        got, latent_query, latent_key, latent_value,
    )
    state_shapes = [((GROUP, HEAD_L), F32)] * 3
    up, down = shift(kv, 1), shift(kv, -1)
    state = call(own_kernel, state_shapes, [VMEM] * 2, queries, kv)
    for step in range(1, size // 2 + 1):
        two = step < size // 2
        blocks = (up, down) if two else (up,)
        if step < size // 2:
            up_next = shift(up, 1)
            down_next = shift(down, -1) if step + 1 < size // 2 else None
        state = call(make_step(step, size, int(two)), state_shapes, [SMEM] + [VMEM] * (4 + len(blocks)), z, queries, *blocks, *state)
        up, down = up_next, down_next
    _, totals, mixed = state
    shares = call(share_kernel, ((plane, SLOTS, width), BF16), [VMEM] * 4, totals, mixed, place, decode_weight)
    arrived = lax.all_to_all(shares, ("ctx", "tp"), split_axis=0, concat_axis=0, tiled=True)
    return call(output_kernel, ((n, width), BF16), [VMEM] * 3, arrived, encoded, members)


def solution(mesh):
    return jax.shard_map(
        per_device,
        mesh=mesh,
        in_specs=(
            P(("bytes", "ctx")),
            P(("bytes", "ctx")),
            P(),
            P(None, "tp"),
            P(None, "tp"),
            P(None, "tp"),
            P(None, ("ctx", "tp")),
            P(None, ("ctx", "tp")),
            P(None, ("ctx", "tp")),
            P(("ctx", "tp"), None),
        ),
        out_specs=P(("bytes", "ctx"), "tp"),
        check_vma=False,
    )
```

```python
import math

import jax
import jax.numpy as jnp
from jax import lax
from jax.experimental import pallas as pl
from jax.experimental.pallas import tpu as pltpu
from jax.sharding import PartitionSpec as P

DB = 1024
HEADS_B = 16
HEAD_L = 128
SLOTS = 72
ROWS = 80
GROUP = 384
KVROWS = 392
SPAN = 4
EPSILON = 1e-06
NEGATIVE = -1e30
F32 = jnp.float32
BF16 = jnp.bfloat16

VMEM = pl.BlockSpec(memory_space=pltpu.VMEM)
SMEM = pl.BlockSpec(memory_space=pltpu.SMEM)


def iota(shape, dim):
    return lax.broadcasted_iota(jnp.int32, shape, dim)


def dot(a, b):
    return jnp.dot(a, b, preferred_element_type=F32)


def dot_nt(a, b):
    return lax.dot_general(a, b, (((1,), (1,)), ((), ())), preferred_element_type=F32)


def dot_tn(a, b):
    return lax.dot_general(a, b, (((0,), (0,)), ((), ())), preferred_element_type=F32)


def table_kernel(table_ref, wq_ref, wk_ref, wv_ref, out_ref):
    embedded = table_ref[...].astype(F32)
    scale = lax.rsqrt(jnp.mean(embedded * embedded, axis=-1, keepdims=True) + EPSILON)
    normed = (embedded * scale).astype(BF16)
    for k, w_ref in enumerate((wq_ref, wk_ref, wv_ref)):
        out_ref[:, 256 * k : 256 * (k + 1)] = dot(normed, w_ref[...]).astype(BF16)


def byte_kernel(block_ref, ids_ref, earlier_ref, offsets_ref, table_ref, enc_ref, member_ref, pay_ref):
    n = ids_ref.shape[1]
    vocab = table_ref.shape[0]
    width = enc_ref.shape[1]
    onehot = (iota((vocab, n), 0) == ids_ref[...]).astype(F32).astype(BF16)
    onehot_e = (iota((vocab, n), 0) == earlier_ref[...]).astype(F32).astype(BF16)
    own = dot_tn(onehot, table_ref[...]).astype(BF16)
    before = dot_tn(onehot_e, table_ref[:, width:]).astype(BF16)
    queries = own[:, :width]
    keys = jnp.concatenate([before[:, :width], own[:, width : 2 * width]], axis=0)
    values = jnp.concatenate([before[:, width:], own[:, 2 * width :]], axis=0)
    query_pos = iota((n, 2 * n), 0)
    key_pos = iota((n, 2 * n), 1)
    first = jnp.where(block_ref[0] > 0, 0, n)
    allowed = (key_pos > query_pos) & (key_pos <= query_pos + n) & (key_pos >= first)
    head = 64
    encoded = jnp.zeros((n, width), F32)
    for h in range(width // head):
        column = iota((1, width), 1)
        mine = ((column >= h * head) & (column < (h + 1) * head)).astype(F32).astype(BF16)
        scores = dot_nt(queries * mine, keys) * (1.0 / math.sqrt(head))
        scores = jnp.where(allowed, scores, NEGATIVE)
        weights = jnp.exp(scores - jnp.max(scores, axis=-1, keepdims=True))
        totals = jnp.sum(weights, axis=-1, keepdims=True)
        encoded = encoded + dot(weights.astype(BF16), values * mine) / totals
    encoded = encoded.astype(BF16)
    enc_ref[...] = encoded
    starts = (offsets_ref[...] == 0).astype(F32)
    upto = (iota((n, n), 0) <= iota((n, n), 1)).astype(F32).astype(BF16)
    running = dot(jnp.broadcast_to(starts, (8, n)).astype(BF16), upto)[0:1]
    patch = running.astype(jnp.int32) - 1
    members = (iota((ROWS, n), 0) == patch).astype(F32)
    member_ref[...] = members.astype(BF16)
    lengths = jnp.sum(members, axis=1, keepdims=True)
    pooled = dot(members.astype(BF16), encoded) / jnp.maximum(lengths, 1.0)
    count = jnp.sum(starts, axis=1, keepdims=True)
    payload = jnp.where(iota((ROWS, width), 0) == SLOTS, count, pooled).astype(BF16)
    for i in range(pay_ref.shape[0]):
        pay_ref[i] = payload


def latent_kernel(core_ref, own_ref, other_ref, wq_ref, wk_ref, wv_ref, q_ref, kv_ref, place_ref):
    blocks = own_ref.shape[0] // 4
    slots = 2 * blocks * ROWS
    is_odd = (core_ref[0] > 0).astype(F32)
    refs = [own_ref] * blocks + [other_ref] * blocks
    here = [r[4 * (k % blocks)][SLOTS : SLOTS + 1, 0:1].astype(F32) for k, r in enumerate(refs)]
    slot = iota((1, slots), 1)
    place = jnp.full((1, slots), -1.0, F32)
    total = jnp.zeros((1, 1), F32)
    for c in range(blocks):
        own, other = here[c], here[blocks + c]
        for k, filled, ahead in ((c, own, total + other * is_odd), (blocks + c, other, total + own * (1.0 - is_odd))):
            order = (slot - ROWS * k).astype(F32)
            place = jnp.where((order >= 0.0) & (order < filled), order + ahead, place)
        total = total + own + other
    place = place.astype(jnp.int32)
    place_ref[...] = jnp.broadcast_to(place, place_ref.shape)
    queries, keys, values = [], [], []
    for k, r in enumerate(refs):
        parts = [r[4 * (k % blocks) + t].astype(F32) for t in range(4)]
        square = sum(jnp.sum(p * p, axis=-1, keepdims=True) for p in parts)
        scale = lax.rsqrt(square * (1.0 / DB) + EPSILON)
        latent = jnp.concatenate([(p * scale).astype(BF16) for p in parts], axis=1)
        queries.append(dot(latent, wq_ref[...]).astype(BF16))
        keys.append(dot(latent, wk_ref[...]).astype(BF16))
        values.append(dot(latent, wv_ref[...]).astype(BF16))
    pick = (iota((GROUP, slots), 0) == place).astype(F32).astype(BF16)
    q_ref[...] = dot(pick, jnp.concatenate(queries, axis=0)).astype(BF16)
    kv_ref[0:GROUP, 0:HEAD_L] = dot(pick, jnp.concatenate(keys, axis=0)).astype(BF16)
    value = dot(pick, jnp.concatenate(values, axis=0))
    largest = jnp.max(jnp.max(jnp.abs(value), axis=1, keepdims=True), axis=0, keepdims=True)
    power = jnp.clip(13.0 - jnp.ceil(jnp.log2(jnp.maximum(largest, 1e-35))), -20.0, 100.0)
    kv_ref[0:GROUP, HEAD_L:] = (value * jnp.exp2(power)).astype(BF16)
    high = total.astype(BF16).astype(F32)
    row = iota((KVROWS - GROUP, 2 * HEAD_L), 0)
    tail = jnp.where(row == 0, high, jnp.where(row == 1, total - high, jnp.where(row == 2, power, 0.0)))
    kv_ref[GROUP:, :] = tail.astype(BF16)


SCALE = 1.0 / (math.sqrt(HEAD_L) * math.log(2.0))


def attend_kernel(z_ref, q_ref, kv_ref, out_ref, m_ref, l_ref, acc_ref):
    m_ref[...] = jnp.full(m_ref.shape, NEGATIVE, F32)
    l_ref[...] = jnp.zeros(l_ref.shape, F32)
    acc_ref[...] = jnp.zeros(acc_ref.shape, F32)
    z = z_ref[0]
    for tile in range(kv_ref.shape[0] // SPAN):

        @pl.when(z >= tile * SPAN)
        def _(tile=tile):
            codes, scores = [], []
            for b in range(tile * SPAN, (tile + 1) * SPAN):
                filled = kv_ref[b, GROUP : GROUP + 1, 0:1].astype(F32) + kv_ref[b, GROUP + 1 : GROUP + 2, 0:1].astype(F32)
                spot = iota((1, GROUP), 1)
                past = jnp.where(spot.astype(F32) < filled, -1, GROUP)
                codes.append(jnp.where(z > b, past, jnp.where(z == b, spot, GROUP)))
                scores.append(dot_nt(q_ref[...], kv_ref[b, 0:GROUP, 0:HEAD_L]))
            code = jnp.concatenate(codes, axis=1)
            score = jnp.concatenate(scores, axis=1) * SCALE
            score = jnp.where(code <= iota((GROUP, 1), 0), score, NEGATIVE)
            old = m_ref[:, 0:1]
            highest = jnp.maximum(old, jnp.max(score, axis=-1, keepdims=True))
            factor = jnp.exp2(old - highest)
            weights = jnp.exp2(score - highest)
            m_ref[...] = jnp.broadcast_to(highest, m_ref.shape)
            l_ref[...] = l_ref[...] * factor + jnp.sum(weights, axis=-1, keepdims=True)
            weights = weights.astype(BF16)
            mixed = acc_ref[...] * factor
            for k in range(SPAN):
                b = tile * SPAN + k
                back = jnp.exp2(-kv_ref[b, GROUP + 2 : GROUP + 3, 0:1].astype(F32))
                mixed = mixed + dot(weights[:, GROUP * k : GROUP * (k + 1)], kv_ref[b, 0:GROUP, HEAD_L:]) * back
            acc_ref[...] = mixed

    out_ref[...] = (acc_ref[...] / l_ref[...]).astype(BF16)


def share_kernel(mixed_ref, place_ref, w_ref, own_ref, other_ref):
    slots = place_ref.shape[1]
    blocks = slots // (2 * ROWS)
    pick = (iota((GROUP, slots), 0) == place_ref[0:1]).astype(F32).astype(BF16)
    spread = dot_tn(pick, mixed_ref[...]).astype(BF16)
    width = own_ref.shape[2]
    for t in range(4):
        part = dot(spread, w_ref[:, width * t : width * (t + 1)]).astype(BF16)
        for c in range(2 * blocks):
            dest_ref = own_ref if c < blocks else other_ref
            dest_ref[4 * (c % blocks) + t] = part[ROWS * c : ROWS * c + SLOTS]


def output_kernel(got_ref, enc_ref, member_ref, out_ref):
    decoded = got_ref[0].astype(F32)
    for h in range(1, got_ref.shape[0]):
        decoded = decoded + got_ref[h].astype(F32)
    decoded = jnp.concatenate([decoded, jnp.zeros((ROWS - SLOTS, decoded.shape[1]), F32)], axis=0)
    high = decoded.astype(BF16)
    low = (decoded - high.astype(F32)).astype(BF16)
    members = member_ref[...]
    out_ref[...] = (enc_ref[...].astype(F32) + dot_tn(members, high) + dot_tn(members, low)).astype(BF16)


def call(kernel, shapes, specs, *args, scratch=()):
    single = not isinstance(shapes, list)
    structs = [jax.ShapeDtypeStruct(s, d) for s, d in ([shapes] if single else shapes)]
    return pl.pallas_call(
        kernel,
        out_shape=structs[0] if single else structs,
        in_specs=specs,
        out_specs=VMEM if single else [VMEM] * len(structs),
        scratch_shapes=scratch,
    )(*args)


def scalar(value):
    return value.astype(jnp.int32).reshape(1)


def swap_cores(value):
    return lax.ppermute(value, "core", [(0, 1), (1, 0)])


def exchange(value):
    return lax.all_to_all(value, ("x", "tp"), split_axis=0, concat_axis=0, tiled=True)


def gather_keys(kv):
    size = lax.axis_size("bytes")
    got = lax.all_gather(kv.astype(jnp.float16), "bytes", axis=0, tiled=True)
    return got.astype(BF16).reshape(size, *kv.shape)


def per_device(ids, offsets, byte_table, byte_query, byte_key, byte_value, latent_query, latent_key, latent_value, decode_weight):
    n = ids.shape[0]
    width = byte_query.shape[1]
    ring = ("bytes", "x", "core")
    plane = lax.axis_size(("x", "tp"))
    earlier = lax.ppermute(ids, ring, [(i, i + 1) for i in range(lax.axis_size(ring) - 1)])
    table = call(table_kernel, ((byte_table.shape[0], 3 * width), BF16), [VMEM] * 4, byte_table, byte_query, byte_key, byte_value)
    encoded, members, payload = call(
        byte_kernel,
        [((n, width), BF16), ((ROWS, n), BF16), ((plane, ROWS, width), BF16)],
        [SMEM] + [VMEM] * 4,
        scalar(lax.axis_index(ring)), ids.reshape(1, n), earlier.reshape(1, n), offsets.reshape(1, n), table,
    )
    own = exchange(payload)
    other = swap_cores(own)
    queries, kv, place = call(
        latent_kernel,
        [((GROUP, HEAD_L), BF16), ((KVROWS, 2 * HEAD_L), BF16), ((8, 2 * ROWS * plane // 4), jnp.int32)],
        [SMEM] + [VMEM] * 5,
        scalar(lax.axis_index("core")), own, other, latent_query, latent_key, latent_value,
    )
    mixed = call(
        attend_kernel,
        ((GROUP, HEAD_L), BF16),
        [SMEM] + [VMEM] * 2,
        scalar(lax.axis_index("bytes")), queries, gather_keys(kv),
        scratch=[pltpu.VMEM((GROUP, HEAD_L), F32)] * 3,
    )
    shape = ((plane, SLOTS, width), BF16)
    mine, theirs = call(share_kernel, [shape, shape], [VMEM] * 3, mixed, place, decode_weight)
    shares = (mine.astype(F32) + swap_cores(theirs).astype(F32)).astype(BF16)
    return call(output_kernel, ((n, width), BF16), [VMEM] * 3, exchange(shares), encoded, members)


def solution(mesh):
    sizes = mesh.shape
    finer = jax.sharding.Mesh(
        mesh.devices.reshape(sizes["bytes"], sizes["ctx"] // 2, 2, sizes["tp"]), ("bytes", "x", "core", "tp")
    )
    rows, heads = ("bytes", "x", "core"), ("x", "core", "tp")
    return jax.shard_map(
        per_device,
        mesh=finer,
        in_specs=(
            P(rows),
            P(rows),
            P(),
            P(None, "tp"),
            P(None, "tp"),
            P(None, "tp"),
            P(None, heads),
            P(None, heads),
            P(None, heads),
            P(heads, None),
        ),
        out_specs=P(rows, "tp"),
        check_vma=False,
    )
```

```python
import math

import jax
import jax.numpy as jnp
from jax import lax
from jax.experimental import pallas as pl
from jax.experimental.pallas import tpu as pltpu
from jax.sharding import PartitionSpec as P

DB = 1024
HEADS_B = 16
HEAD_L = 128
SLOTS = 72
ROWS = 72
UNUSED = 1e9
GROUP = 384
KVROWS = 392
SPAN = 4
EPSILON = 1e-06
NEGATIVE = -1e30
F32 = jnp.float32
BF16 = jnp.bfloat16

VMEM = pl.BlockSpec(memory_space=pltpu.VMEM)
SMEM = pl.BlockSpec(memory_space=pltpu.SMEM)


def iota(shape, dim):
    return lax.broadcasted_iota(jnp.int32, shape, dim)


def dot(a, b):
    return jnp.dot(a, b, preferred_element_type=F32)


def dot_nt(a, b):
    return lax.dot_general(a, b, (((1,), (1,)), ((), ())), preferred_element_type=F32)


def dot_tn(a, b):
    return lax.dot_general(a, b, (((0,), (0,)), ((), ())), preferred_element_type=F32)


def table_kernel(table_ref, wq_ref, wk_ref, wv_ref, out_ref):
    embedded = table_ref[...].astype(F32)
    scale = lax.rsqrt(jnp.mean(embedded * embedded, axis=-1, keepdims=True) + EPSILON)
    normed = (embedded * scale).astype(BF16)
    for k, w_ref in enumerate((wq_ref, wk_ref, wv_ref)):
        out_ref[:, 256 * k : 256 * (k + 1)] = dot(normed, w_ref[...]).astype(BF16)


def byte_kernel(block_ref, ids_ref, earlier_ref, offsets_ref, table_ref, enc_ref, member_ref, pay_ref):
    n = ids_ref.shape[1]
    vocab = table_ref.shape[0]
    width = enc_ref.shape[1]
    onehot = (iota((vocab, n), 0) == ids_ref[...]).astype(F32).astype(BF16)
    onehot_e = (iota((vocab, n), 0) == earlier_ref[...]).astype(F32).astype(BF16)
    own = dot_tn(onehot, table_ref[...]).astype(BF16)
    before = dot_tn(onehot_e, table_ref[:, width:]).astype(BF16)
    queries = own[:, :width]
    keys = jnp.concatenate([before[:, :width], own[:, width : 2 * width]], axis=0)
    values = jnp.concatenate([before[:, width:], own[:, 2 * width :]], axis=0)
    query_pos = iota((n, 2 * n), 0)
    key_pos = iota((n, 2 * n), 1)
    first = jnp.where(block_ref[0] > 0, 0, n)
    allowed = (key_pos > query_pos) & (key_pos <= query_pos + n) & (key_pos >= first)
    head = 64
    encoded = jnp.zeros((n, width), F32)
    for h in range(width // head):
        column = iota((1, width), 1)
        mine = ((column >= h * head) & (column < (h + 1) * head)).astype(F32).astype(BF16)
        scores = dot_nt(queries * mine, keys) * (1.0 / math.sqrt(head))
        scores = jnp.where(allowed, scores, NEGATIVE)
        weights = jnp.exp(scores - jnp.max(scores, axis=-1, keepdims=True))
        totals = jnp.sum(weights, axis=-1, keepdims=True)
        encoded = encoded + dot(weights.astype(BF16), values * mine) / totals
    encoded = encoded.astype(BF16)
    enc_ref[...] = encoded
    starts = (offsets_ref[...] == 0).astype(F32)
    upto = (iota((n, n), 0) <= iota((n, n), 1)).astype(F32).astype(BF16)
    running = dot(jnp.broadcast_to(starts, (8, n)).astype(BF16), upto)[0:1]
    patch = running.astype(jnp.int32) - 1
    members = (iota((ROWS, n), 0) == patch).astype(F32)
    member_ref[...] = members.astype(BF16)
    lengths = jnp.sum(members, axis=1, keepdims=True)
    pooled = dot(members.astype(BF16), encoded) / jnp.maximum(lengths, 1.0)
    empty = (lengths < 0.5) & (iota((ROWS, width), 1) == 0)
    payload = jnp.where(empty, UNUSED, pooled).astype(BF16)
    for i in range(pay_ref.shape[0]):
        pay_ref[i] = payload


def latent_kernel(core_ref, own_ref, other_ref, wq_ref, wk_ref, wv_ref, q_ref, kv_ref, place_ref):
    blocks = own_ref.shape[0] // 4
    slots = 2 * blocks * ROWS
    is_odd = (core_ref[0] > 0).astype(F32)
    weight = jnp.concatenate([wq_ref[...], wk_ref[...], wv_ref[...]], axis=1)
    here, rows = [], []
    for r in (own_ref, other_ref):
        for k in range(blocks):
            parts = [r[4 * k + t].astype(F32) for t in range(4)]
            used = (parts[0][:, 0:1] < 0.1 * UNUSED).astype(F32)
            here.append(jnp.sum(used, axis=0, keepdims=True))
            square = sum(jnp.sum(p * p, axis=-1, keepdims=True) for p in parts)
            scale = used * lax.rsqrt(square * (1.0 / DB) + EPSILON)
            rows.append(jnp.concatenate([(p * scale).astype(BF16) for p in parts], axis=1))
    made = dot(jnp.concatenate(rows, axis=0), weight).astype(BF16)
    slot = iota((1, slots), 1)
    place = jnp.full((1, slots), -1.0, F32)
    total = jnp.zeros((1, 1), F32)
    for c in range(blocks):
        own, other = here[c], here[blocks + c]
        for k, filled, ahead in ((c, own, total + other * is_odd), (blocks + c, other, total + own * (1.0 - is_odd))):
            order = (slot - ROWS * k).astype(F32)
            place = jnp.where((order >= 0.0) & (order < filled), order + ahead, place)
        total = total + own + other
    place = place.astype(jnp.int32)
    place_ref[...] = jnp.broadcast_to(place, place_ref.shape)
    pick = (iota((GROUP, slots), 0) == place).astype(F32).astype(BF16)
    packed = dot(pick, made)
    q_ref[...] = packed[:, 0:HEAD_L].astype(BF16)
    kv_ref[0:GROUP, 0:HEAD_L] = packed[:, HEAD_L : 2 * HEAD_L].astype(BF16)
    value = packed[:, 2 * HEAD_L :]
    largest = jnp.max(jnp.max(jnp.abs(value), axis=1, keepdims=True), axis=0, keepdims=True)
    power = jnp.clip(13.0 - jnp.ceil(jnp.log2(jnp.maximum(largest, 1e-35))), -20.0, 100.0)
    kv_ref[0:GROUP, HEAD_L:] = (value * jnp.exp2(power)).astype(BF16)
    high = total.astype(BF16).astype(F32)
    row = iota((KVROWS - GROUP, 2 * HEAD_L), 0)
    tail = jnp.where(row == 0, high, jnp.where(row == 1, total - high, jnp.where(row == 2, power, 0.0)))
    kv_ref[GROUP:, :] = tail.astype(BF16)


SCALE = 1.0 / (math.sqrt(HEAD_L) * math.log(2.0))


def attend_kernel(z_ref, q_ref, kv_ref, place_ref, w_ref, out_ref, theirs_ref, m_ref, l_ref, acc_ref):
    m_ref[...] = jnp.full(m_ref.shape, NEGATIVE, F32)
    l_ref[...] = jnp.zeros(l_ref.shape, F32)
    acc_ref[...] = jnp.zeros(acc_ref.shape, F32)
    z = z_ref[0]
    for tile in range(kv_ref.shape[0] // SPAN):

        @pl.when(z >= tile * SPAN)
        def _(tile=tile):
            codes, scores = [], []
            for b in range(tile * SPAN, (tile + 1) * SPAN):
                filled = kv_ref[b, GROUP : GROUP + 1, 0:1].astype(F32) + kv_ref[b, GROUP + 1 : GROUP + 2, 0:1].astype(F32)
                spot = iota((1, GROUP), 1)
                past = jnp.where(spot.astype(F32) < filled, -1, GROUP)
                codes.append(jnp.where(z > b, past, jnp.where(z == b, spot, GROUP)))
                scores.append(dot_nt(q_ref[...], kv_ref[b, 0:GROUP, 0:HEAD_L]))
            code = jnp.concatenate(codes, axis=1)
            score = jnp.concatenate(scores, axis=1) * SCALE
            score = jnp.where(code <= iota((GROUP, 1), 0), score, NEGATIVE)
            old = m_ref[:, 0:1]
            highest = jnp.maximum(old, jnp.max(score, axis=-1, keepdims=True))
            factor = jnp.exp2(old - highest)
            weights = jnp.exp2(score - highest)
            m_ref[...] = jnp.broadcast_to(highest, m_ref.shape)
            l_ref[...] = l_ref[...] * factor + jnp.sum(weights, axis=-1, keepdims=True)
            weights = weights.astype(BF16)
            mixed = acc_ref[...] * factor
            for k in range(SPAN):
                b = tile * SPAN + k
                back = jnp.exp2(-kv_ref[b, GROUP + 2 : GROUP + 3, 0:1].astype(F32))
                mixed = mixed + dot(weights[:, GROUP * k : GROUP * (k + 1)], kv_ref[b, 0:GROUP, HEAD_L:]) * back
            acc_ref[...] = mixed

    mixed = (acc_ref[...] / l_ref[...]).astype(BF16)
    out_ref[...] = mixed
    write_shares(mixed, place_ref, w_ref, theirs_ref, 1)


def write_shares(mixed, place_ref, w_ref, shares_ref, half):
    slots = place_ref.shape[1] // 2
    place = place_ref[0:1][:, slots * half : slots * (half + 1)]
    pick = (iota((GROUP, slots), 0) == place).astype(F32).astype(BF16)
    spread = dot_tn(pick, mixed).astype(BF16)
    width = shares_ref.shape[2]
    for t in range(4):
        part = dot(spread, w_ref[:, width * t : width * (t + 1)]).astype(BF16)
        for c in range(slots // ROWS):
            shares_ref[4 * c + t] = part[ROWS * c : ROWS * (c + 1)]


def share_kernel(mixed_ref, place_ref, w_ref, mine_ref):
    write_shares(mixed_ref[...], place_ref, w_ref, mine_ref, 0)


def output_kernel(got_ref, enc_ref, member_ref, out_ref):
    decoded = got_ref[0].astype(F32)
    for h in range(1, got_ref.shape[0]):
        decoded = decoded + got_ref[h].astype(F32)
    high = decoded.astype(BF16)
    low = (decoded - high.astype(F32)).astype(BF16)
    members = member_ref[...]
    out_ref[...] = (enc_ref[...].astype(F32) + dot_tn(members, high) + dot_tn(members, low)).astype(BF16)


def call(kernel, shapes, specs, *args, scratch=(), grant=16):
    single = not isinstance(shapes, list)
    structs = [jax.ShapeDtypeStruct(s, d) for s, d in ([shapes] if single else shapes)]
    return pl.pallas_call(
        kernel,
        out_shape=structs[0] if single else structs,
        in_specs=specs,
        out_specs=VMEM if single else [VMEM] * len(structs),
        scratch_shapes=scratch,
        compiler_params=pltpu.CompilerParams(vmem_limit_bytes=grant << 20),
    )(*args)


def scalar(value):
    return value.astype(jnp.int32).reshape(1)


def swap_cores(value):
    return lax.ppermute(value, "core", [(0, 1), (1, 0)])


def exchange(value):
    return lax.all_to_all(value, ("x", "tp"), split_axis=0, concat_axis=0, tiled=True)


def gather_keys(kv):
    size = lax.axis_size("bytes")
    got = lax.all_gather(kv.astype(jnp.float16), "bytes", axis=0, tiled=True)
    return got.astype(BF16).reshape(size, *kv.shape)


def per_device(ids, offsets, byte_table, byte_query, byte_key, byte_value, latent_query, latent_key, latent_value, decode_weight):
    n = ids.shape[0]
    width = byte_query.shape[1]
    ring = ("bytes", "x", "core")
    plane = lax.axis_size(("x", "tp"))
    earlier = lax.ppermute(ids, ring, [(i, i + 1) for i in range(lax.axis_size(ring) - 1)])
    table = call(table_kernel, ((byte_table.shape[0], 3 * width), BF16), [VMEM] * 4, byte_table, byte_query, byte_key, byte_value)
    encoded, members, payload = call(
        byte_kernel,
        [((n, width), BF16), ((ROWS, n), BF16), ((plane, ROWS, width), BF16)],
        [SMEM] + [VMEM] * 4,
        scalar(lax.axis_index(ring)), ids.reshape(1, n), earlier.reshape(1, n), offsets.reshape(1, n), table,
    )
    own = exchange(payload)
    other = swap_cores(own)
    queries, kv, place = call(
        latent_kernel,
        [((GROUP, HEAD_L), BF16), ((KVROWS, 2 * HEAD_L), BF16), ((8, 2 * ROWS * plane // 4), jnp.int32)],
        [SMEM] + [VMEM] * 5,
        scalar(lax.axis_index("core")), own, other, latent_query, latent_key, latent_value,
    )
    shape = ((plane, SLOTS, width), BF16)
    mixed, theirs = call(
        attend_kernel,
        [((GROUP, HEAD_L), BF16), shape],
        [SMEM] + [VMEM] * 4,
        scalar(lax.axis_index("bytes")), queries, gather_keys(kv), place, decode_weight,
        scratch=[pltpu.VMEM((GROUP, HEAD_L), F32)] * 3, grant=32,
    )
    mine = call(share_kernel, shape, [VMEM] * 3, mixed, place, decode_weight)
    shares = (mine.astype(F32) + swap_cores(theirs).astype(F32)).astype(BF16)
    return call(output_kernel, ((n, width), BF16), [VMEM] * 3, exchange(shares), encoded, members)


def solution(mesh):
    sizes = mesh.shape
    finer = jax.sharding.Mesh(
        mesh.devices.reshape(sizes["bytes"], sizes["ctx"] // 2, 2, sizes["tp"]), ("bytes", "x", "core", "tp")
    )
    rows, heads = ("bytes", "x", "core"), ("x", "core", "tp")
    return jax.shard_map(
        per_device,
        mesh=finer,
        in_specs=(
            P(rows),
            P(rows),
            P(),
            P(None, "tp"),
            P(None, "tp"),
            P(None, "tp"),
            P(None, heads),
            P(None, heads),
            P(None, heads),
            P(heads, None),
        ),
        out_specs=P(rows, "tp"),
        check_vma=False,
    )
```

```python
import math

import jax
import jax.numpy as jnp
from jax import lax
from jax.experimental import pallas as pl
from jax.experimental.pallas import tpu as pltpu
from jax.sharding import PartitionSpec as P

DB = 1024
HEADS_B = 16
HEAD_L = 128
SLOTS = 72
ROWS = 72
UNUSED = 1e9
GROUP = 384
KVROWS = 392
SPAN = 4
EPSILON = 1e-06
NEGATIVE = -1e30
F32 = jnp.float32
BF16 = jnp.bfloat16

VMEM = pl.BlockSpec(memory_space=pltpu.VMEM)
SMEM = pl.BlockSpec(memory_space=pltpu.SMEM)


def iota(shape, dim):
    return lax.broadcasted_iota(jnp.int32, shape, dim)


def dot(a, b):
    return jnp.dot(a, b, preferred_element_type=F32)


def dot_nt(a, b):
    return lax.dot_general(a, b, (((1,), (1,)), ((), ())), preferred_element_type=F32)


def dot_tn(a, b):
    return lax.dot_general(a, b, (((0,), (0,)), ((), ())), preferred_element_type=F32)


PIECES = 4


def table_kernel(table_hbm, wq_hbm, wk_hbm, wv_hbm, out_ref, table_ref, wq_ref, wk_ref, wv_ref, sems):
    pairs = ((table_hbm, table_ref), (wq_hbm, wq_ref), (wk_hbm, wk_ref), (wv_hbm, wv_ref))
    copies = []
    for k, (source, target) in enumerate(pairs):
        rows = source.shape[0] // PIECES
        part = [pl.ds(rows * i, rows) for i in range(PIECES)]
        copies.append([pltpu.make_async_copy(source.at[p], target.at[p], sems.at[k, i]) for i, p in enumerate(part)])
        for copy in copies[-1]:
            copy.start()
    for copy in copies[0]:
        copy.wait()
    embedded = table_ref[...].astype(F32)
    scale = lax.rsqrt(jnp.mean(embedded * embedded, axis=-1, keepdims=True) + EPSILON)
    normed = (embedded * scale).astype(BF16)
    width = wq_ref.shape[1]
    for k, w_ref in enumerate((wq_ref, wk_ref, wv_ref)):
        for copy in copies[k + 1]:
            copy.wait()
        out_ref[:, width * k : width * (k + 1)] = dot(normed, w_ref[...]).astype(BF16)


def byte_kernel(block_ref, ids_ref, earlier_ref, offsets_ref, table_ref, enc_ref, member_ref, pay_ref):
    n = ids_ref.shape[1]
    vocab = table_ref.shape[0]
    width = enc_ref.shape[1]
    onehot = (iota((vocab, n), 0) == ids_ref[...]).astype(F32).astype(BF16)
    onehot_e = (iota((vocab, n), 0) == earlier_ref[...]).astype(F32).astype(BF16)
    own = dot_tn(onehot, table_ref[...]).astype(BF16)
    before = dot_tn(onehot_e, table_ref[:, width:]).astype(BF16)
    queries = own[:, :width]
    keys = jnp.concatenate([before[:, :width], own[:, width : 2 * width]], axis=0)
    values = jnp.concatenate([before[:, width:], own[:, 2 * width :]], axis=0)
    query_pos = iota((n, 2 * n), 0)
    key_pos = iota((n, 2 * n), 1)
    first = jnp.where(block_ref[0] > 0, 0, n)
    allowed = (key_pos > query_pos) & (key_pos <= query_pos + n) & (key_pos >= first)
    head = 64
    encoded = jnp.zeros((n, width), F32)
    for h in range(width // head):
        column = iota((1, width), 1)
        mine = ((column >= h * head) & (column < (h + 1) * head)).astype(F32).astype(BF16)
        scores = dot_nt(queries * mine, keys) * (1.0 / math.sqrt(head))
        scores = jnp.where(allowed, scores, NEGATIVE)
        weights = jnp.exp(scores - jnp.max(scores, axis=-1, keepdims=True))
        totals = jnp.sum(weights, axis=-1, keepdims=True)
        encoded = encoded + dot(weights.astype(BF16), values * mine) / totals
    encoded = encoded.astype(BF16)
    enc_ref[...] = encoded
    starts = (offsets_ref[...] == 0).astype(F32)
    upto = (iota((n, n), 0) <= iota((n, n), 1)).astype(F32).astype(BF16)
    running = dot(jnp.broadcast_to(starts, (8, n)).astype(BF16), upto)[0:1]
    patch = running.astype(jnp.int32) - 1
    members = (iota((ROWS, n), 0) == patch).astype(F32)
    member_ref[...] = members.astype(BF16)
    lengths = jnp.sum(members, axis=1, keepdims=True)
    pooled = dot(members.astype(BF16), encoded) / jnp.maximum(lengths, 1.0)
    empty = (lengths < 0.5) & (iota((ROWS, width), 1) == 0)
    payload = jnp.where(empty, UNUSED, pooled).astype(BF16)
    for i in range(pay_ref.shape[0]):
        pay_ref[i] = payload


def project_blocks(got_ref, wq_ref, wk_ref, wv_ref):
    weight = jnp.concatenate([wq_ref[...], wk_ref[...], wv_ref[...]], axis=1)
    here, rows = [], []
    for k in range(got_ref.shape[0] // 4):
        parts = [got_ref[4 * k + t].astype(F32) for t in range(4)]
        used = (parts[0][:, 0:1] < 0.1 * UNUSED).astype(F32)
        here.append(jnp.sum(used, axis=0, keepdims=True))
        square = sum(jnp.sum(p * p, axis=-1, keepdims=True) for p in parts)
        scale = used * lax.rsqrt(square * (1.0 / DB) + EPSILON)
        rows.append(jnp.concatenate([(p * scale).astype(BF16) for p in parts], axis=1))
    return here, dot(jnp.concatenate(rows, axis=0), weight).astype(BF16)


def own_latent_kernel(own_ref, wq_ref, wk_ref, wv_ref, made_ref, count_ref):
    here, made = project_blocks(own_ref, wq_ref, wk_ref, wv_ref)
    made_ref[...] = made
    for k, filled in enumerate(here):
        count_ref[k : k + 1] = jnp.broadcast_to(filled, (1, count_ref.shape[1]))


def latent_kernel(core_ref, made_ref, count_ref, other_ref, wq_ref, wk_ref, wv_ref, q_ref, kv_ref, place_ref):
    blocks = other_ref.shape[0] // 4
    slots = 2 * blocks * ROWS
    is_odd = (core_ref[0] > 0).astype(F32)
    here, made = project_blocks(other_ref, wq_ref, wk_ref, wv_ref)
    here = [count_ref[k : k + 1, 0:1] for k in range(blocks)] + here
    made = jnp.concatenate([made_ref[...], made], axis=0)
    slot = iota((1, slots), 1)
    place = jnp.full((1, slots), -1.0, F32)
    total = jnp.zeros((1, 1), F32)
    for c in range(blocks):
        own, other = here[c], here[blocks + c]
        for k, filled, ahead in ((c, own, total + other * is_odd), (blocks + c, other, total + own * (1.0 - is_odd))):
            order = (slot - ROWS * k).astype(F32)
            place = jnp.where((order >= 0.0) & (order < filled), order + ahead, place)
        total = total + own + other
    place = place.astype(jnp.int32)
    place_ref[...] = jnp.broadcast_to(place, place_ref.shape)
    pick = (iota((GROUP, slots), 0) == place).astype(F32).astype(BF16)
    packed = dot(pick, made)
    q_ref[...] = packed[:, 0:HEAD_L].astype(BF16)
    kv_ref[0:GROUP, 0:HEAD_L] = packed[:, HEAD_L : 2 * HEAD_L].astype(BF16)
    value = packed[:, 2 * HEAD_L :]
    largest = jnp.max(jnp.max(jnp.abs(value), axis=1, keepdims=True), axis=0, keepdims=True)
    power = jnp.clip(13.0 - jnp.ceil(jnp.log2(jnp.maximum(largest, 1e-35))), -20.0, 100.0)
    kv_ref[0:GROUP, HEAD_L:] = (value * jnp.exp2(power)).astype(BF16)
    high = total.astype(BF16).astype(F32)
    row = iota((KVROWS - GROUP, 2 * HEAD_L), 0)
    tail = jnp.where(row == 0, high, jnp.where(row == 1, total - high, jnp.where(row == 2, power, 0.0)))
    kv_ref[GROUP:, :] = tail.astype(BF16)


SCALE = 1.0 / (math.sqrt(HEAD_L) * math.log(2.0))


def attend_kernel(z_ref, q_ref, kv_ref, place_ref, w_ref, out_ref, theirs_ref, m_ref, l_ref, acc_ref):
    m_ref[...] = jnp.full(m_ref.shape, NEGATIVE, F32)
    l_ref[...] = jnp.zeros(l_ref.shape, F32)
    acc_ref[...] = jnp.zeros(acc_ref.shape, F32)
    z = z_ref[0]
    for tile in range(kv_ref.shape[0] // SPAN):

        @pl.when(z >= tile * SPAN)
        def _(tile=tile):
            codes, scores = [], []
            for b in range(tile * SPAN, (tile + 1) * SPAN):
                filled = kv_ref[b, GROUP : GROUP + 1, 0:1].astype(F32) + kv_ref[b, GROUP + 1 : GROUP + 2, 0:1].astype(F32)
                spot = iota((1, GROUP), 1)
                past = jnp.where(spot.astype(F32) < filled, -1, GROUP)
                codes.append(jnp.where(z > b, past, jnp.where(z == b, spot, GROUP)))
                scores.append(dot_nt(q_ref[...], kv_ref[b, 0:GROUP, 0:HEAD_L]))
            code = jnp.concatenate(codes, axis=1)
            score = jnp.concatenate(scores, axis=1) * SCALE
            score = jnp.where(code <= iota((GROUP, 1), 0), score, NEGATIVE)
            old = m_ref[:, 0:1]
            highest = jnp.maximum(old, jnp.max(score, axis=-1, keepdims=True))
            factor = jnp.exp2(old - highest)
            weights = jnp.exp2(score - highest)
            m_ref[...] = jnp.broadcast_to(highest, m_ref.shape)
            l_ref[...] = l_ref[...] * factor + jnp.sum(weights, axis=-1, keepdims=True)
            weights = weights.astype(BF16)
            mixed = acc_ref[...] * factor
            for k in range(SPAN):
                b = tile * SPAN + k
                back = jnp.exp2(-kv_ref[b, GROUP + 2 : GROUP + 3, 0:1].astype(F32))
                mixed = mixed + dot(weights[:, GROUP * k : GROUP * (k + 1)], kv_ref[b, 0:GROUP, HEAD_L:]) * back
            acc_ref[...] = mixed

    mixed = (acc_ref[...] / l_ref[...]).astype(BF16)
    out_ref[...] = mixed
    write_shares(mixed, place_ref, w_ref, theirs_ref, 1)


def write_shares(mixed, place_ref, w_ref, shares_ref, half):
    slots = place_ref.shape[1] // 2
    place = place_ref[0:1][:, slots * half : slots * (half + 1)]
    pick = (iota((GROUP, slots), 0) == place).astype(F32).astype(BF16)
    spread = dot_tn(pick, mixed).astype(BF16)
    width = shares_ref.shape[2]
    for t in range(4):
        part = dot(spread, w_ref[:, width * t : width * (t + 1)]).astype(BF16)
        for c in range(slots // ROWS):
            shares_ref[4 * c + t] = part[ROWS * c : ROWS * (c + 1)]


def share_kernel(mixed_ref, place_ref, w_ref, mine_ref):
    write_shares(mixed_ref[...], place_ref, w_ref, mine_ref, 0)


def output_kernel(got_ref, enc_ref, member_ref, out_ref):
    decoded = got_ref[0].astype(F32)
    for h in range(1, got_ref.shape[0]):
        decoded = decoded + got_ref[h].astype(F32)
    high = decoded.astype(BF16)
    low = (decoded - high.astype(F32)).astype(BF16)
    members = member_ref[...]
    out_ref[...] = (enc_ref[...].astype(F32) + dot_tn(members, high) + dot_tn(members, low)).astype(BF16)


def call(kernel, shapes, specs, *args, scratch=(), grant=16):
    single = not isinstance(shapes, list)
    structs = [jax.ShapeDtypeStruct(s, d) for s, d in ([shapes] if single else shapes)]
    return pl.pallas_call(
        kernel,
        out_shape=structs[0] if single else structs,
        in_specs=specs,
        out_specs=VMEM if single else [VMEM] * len(structs),
        scratch_shapes=scratch,
        compiler_params=pltpu.CompilerParams(vmem_limit_bytes=grant << 20),
    )(*args)


def scalar(value):
    return value.astype(jnp.int32).reshape(1)


def swap_cores(value):
    return lax.ppermute(value, "core", [(0, 1), (1, 0)])


def exchange(value):
    return lax.all_to_all(value, ("x", "tp"), split_axis=0, concat_axis=0, tiled=True)


def gather_keys(kv):
    size = lax.axis_size("bytes")
    got = lax.all_gather(kv.astype(jnp.float16), "bytes", axis=0, tiled=True)
    return got.astype(BF16).reshape(size, *kv.shape)


def per_device(ids, offsets, byte_table, byte_query, byte_key, byte_value, latent_query, latent_key, latent_value, decode_weight):
    n = ids.shape[0]
    width = byte_query.shape[1]
    ring = ("bytes", "x", "core")
    plane = lax.axis_size(("x", "tp"))
    earlier = lax.ppermute(ids, ring, [(i, i + 1) for i in range(lax.axis_size(ring) - 1)])
    weights = [pltpu.with_memory_space_constraint(w, pltpu.HBM) for w in (byte_table, byte_query, byte_key, byte_value)]
    table = call(
        table_kernel,
        ((byte_table.shape[0], 3 * width), BF16),
        [pl.BlockSpec(memory_space=pltpu.HBM)] * 4,
        *weights,
        scratch=[pltpu.VMEM(w.shape, BF16) for w in weights] + [pltpu.SemaphoreType.DMA((4, PIECES))],
    )
    encoded, members, payload = call(
        byte_kernel,
        [((n, width), BF16), ((ROWS, n), BF16), ((plane, ROWS, width), BF16)],
        [SMEM] + [VMEM] * 4,
        scalar(lax.axis_index(ring)), ids.reshape(1, n), earlier.reshape(1, n), offsets.reshape(1, n), table,
    )
    own = exchange(payload)
    other = swap_cores(own)
    projections = (latent_query, latent_key, latent_value)
    half = ROWS * plane // 4
    made, counts = call(
        own_latent_kernel, [((half, 3 * HEAD_L), BF16), ((8, HEAD_L), F32)], [VMEM] * 4, own, *projections
    )
    queries, kv, place = call(
        latent_kernel,
        [((GROUP, HEAD_L), BF16), ((KVROWS, 2 * HEAD_L), BF16), ((8, 2 * half), jnp.int32)],
        [SMEM] + [VMEM] * 6,
        scalar(lax.axis_index("core")), made, counts, other, *projections,
    )
    shape = ((plane, SLOTS, width), BF16)
    mixed, theirs = call(
        attend_kernel,
        [((GROUP, HEAD_L), BF16), shape],
        [SMEM] + [VMEM] * 4,
        scalar(lax.axis_index("bytes")), queries, gather_keys(kv), place, decode_weight,
        scratch=[pltpu.VMEM((GROUP, HEAD_L), F32)] * 3, grant=32,
    )
    mine = call(share_kernel, shape, [VMEM] * 3, mixed, place, decode_weight)
    shares = (mine.astype(F32) + swap_cores(theirs).astype(F32)).astype(BF16)
    return call(output_kernel, ((n, width), BF16), [VMEM] * 3, exchange(shares), encoded, members)


def solution(mesh):
    sizes = mesh.shape
    finer = jax.sharding.Mesh(
        mesh.devices.reshape(sizes["bytes"], sizes["ctx"] // 2, 2, sizes["tp"]), ("bytes", "x", "core", "tp")
    )
    rows, heads = ("bytes", "x", "core"), ("x", "core", "tp")
    return jax.shard_map(
        per_device,
        mesh=finer,
        in_specs=(
            P(rows),
            P(rows),
            P(),
            P(None, "tp"),
            P(None, "tp"),
            P(None, "tp"),
            P(None, heads),
            P(None, heads),
            P(None, heads),
            P(heads, None),
        ),
        out_specs=P(rows, "tp"),
        check_vma=False,
    )
```

```python
import math

import jax
import jax.numpy as jnp
from jax import lax
from jax.experimental import pallas as pl
from jax.experimental.pallas import tpu as pltpu
from jax.sharding import PartitionSpec as P

DB = 1024
HEADS_B = 16
HEAD_L = 128
SLOTS = 72
ROWS = 72
UNUSED = 1e9
GROUP = 384
KVROWS = 392
SPANS = (1, 3, 4, 4, 4)
EPSILON = 1e-06
NEGATIVE = -1e30
F32 = jnp.float32
BF16 = jnp.bfloat16

VMEM = pl.BlockSpec(memory_space=pltpu.VMEM)
SMEM = pl.BlockSpec(memory_space=pltpu.SMEM)


def iota(shape, dim):
    return lax.broadcasted_iota(jnp.int32, shape, dim)


def dot(a, b):
    return jnp.dot(a, b, preferred_element_type=F32)


def dot_nt(a, b):
    return lax.dot_general(a, b, (((1,), (1,)), ((), ())), preferred_element_type=F32)


def dot_tn(a, b):
    return lax.dot_general(a, b, (((0,), (0,)), ((), ())), preferred_element_type=F32)


PIECES = 4


def table_kernel(table_hbm, wq_hbm, wk_hbm, wv_hbm, out_ref, table_ref, wq_ref, wk_ref, wv_ref, sems):
    pairs = ((table_hbm, table_ref), (wq_hbm, wq_ref), (wk_hbm, wk_ref), (wv_hbm, wv_ref))
    copies = []
    for k, (source, target) in enumerate(pairs):
        rows = source.shape[0] // PIECES
        part = [pl.ds(rows * i, rows) for i in range(PIECES)]
        copies.append([pltpu.make_async_copy(source.at[p], target.at[p], sems.at[k, i]) for i, p in enumerate(part)])
        for copy in copies[-1]:
            copy.start()
    for copy in copies[0]:
        copy.wait()
    embedded = table_ref[...].astype(F32)
    scale = lax.rsqrt(jnp.mean(embedded * embedded, axis=-1, keepdims=True) + EPSILON)
    normed = (embedded * scale).astype(BF16)
    width = wq_ref.shape[1]
    for k, w_ref in enumerate((wq_ref, wk_ref, wv_ref)):
        for copy in copies[k + 1]:
            copy.wait()
        out_ref[:, width * k : width * (k + 1)] = dot(normed, w_ref[...]).astype(BF16)


HEAD_B = 64


def head_column(width, h):
    column = iota((1, width), 1)
    return ((column >= h * HEAD_B) & (column < (h + 1) * HEAD_B)).astype(F32).astype(BF16)


def spread_heads(columns, width):
    which = iota((1, width), 1) // HEAD_B
    out = jnp.broadcast_to(columns[0], (columns[0].shape[0], width))
    for h in range(1, len(columns)):
        out = jnp.where(which == h, columns[h], out)
    return out


def own_byte_kernel(ids_ref, offsets_ref, table_ref, q_ref, acc_ref, stat_ref, member_ref):
    n = ids_ref.shape[1]
    width = q_ref.shape[1]
    onehot = (iota((table_ref.shape[0], n), 0) == ids_ref[...]).astype(F32).astype(BF16)
    own = dot_tn(onehot, table_ref[...]).astype(BF16)
    queries, keys, values = own[:, :width], own[:, width : 2 * width], own[:, 2 * width :]
    q_ref[...] = queries
    causal = iota((n, n), 1) <= iota((n, n), 0)
    lane = iota((1, stat_ref.shape[1]), 1)
    stats = jnp.zeros(stat_ref.shape, F32)
    mixed = jnp.zeros((n, width), F32)
    heads = width // HEAD_B
    for h in range(heads):
        mine = head_column(width, h)
        scores = jnp.where(causal, dot_nt(queries * mine, keys) * (1.0 / math.sqrt(HEAD_B)), NEGATIVE)
        highest = jnp.max(scores, axis=-1, keepdims=True)
        weights = jnp.exp(scores - highest)
        stats = jnp.where(lane == h, highest, stats)
        stats = jnp.where(lane == heads + h, jnp.sum(weights, axis=-1, keepdims=True), stats)
        mixed = mixed + dot(weights.astype(BF16), values * mine)
    acc_ref[...] = mixed
    stat_ref[...] = stats
    starts = (offsets_ref[...] == 0).astype(F32)
    upto = (iota((n, n), 0) <= iota((n, n), 1)).astype(F32).astype(BF16)
    running = dot(jnp.broadcast_to(starts, (8, n)).astype(BF16), upto)[0:1]
    patch = running.astype(jnp.int32) - 1
    member_ref[...] = (iota((ROWS, n), 0) == patch).astype(F32).astype(BF16)


def byte_kernel(block_ref, earlier_ref, table_ref, q_ref, acc_ref, stat_ref, member_ref, enc_ref, pay_ref):
    n, width = q_ref.shape
    onehot = (iota((table_ref.shape[0], n), 0) == earlier_ref[...]).astype(F32).astype(BF16)
    before = dot_tn(onehot, table_ref[:, width:]).astype(BF16)
    keys, values = before[:, :width], before[:, width:]
    first = jnp.where(block_ref[0] > 0, 0, n)
    allowed = (iota((n, n), 1) > iota((n, n), 0)) & (iota((n, n), 1) >= first)
    queries = q_ref[...]
    heads = width // HEAD_B
    mixed = jnp.zeros((n, width), F32)
    factors, totals = [], []
    for h in range(heads):
        mine = head_column(width, h)
        scores = jnp.where(allowed, dot_nt(queries * mine, keys) * (1.0 / math.sqrt(HEAD_B)), NEGATIVE)
        old = stat_ref[:, h : h + 1]
        highest = jnp.maximum(old, jnp.max(scores, axis=-1, keepdims=True))
        weights = jnp.exp(scores - highest)
        factors.append(jnp.exp(old - highest))
        totals.append(stat_ref[:, heads + h : heads + h + 1] * factors[-1] + jnp.sum(weights, axis=-1, keepdims=True))
        mixed = mixed + dot(weights.astype(BF16), values * mine)
    mixed = mixed + acc_ref[...] * spread_heads(factors, width)
    encoded = (mixed / spread_heads(totals, width)).astype(BF16)
    enc_ref[...] = encoded
    members = member_ref[...]
    lengths = jnp.sum(members.astype(F32), axis=1, keepdims=True)
    pooled = dot(members, encoded) / jnp.maximum(lengths, 1.0)
    empty = (lengths < 0.5) & (iota((ROWS, width), 1) == 0)
    payload = jnp.where(empty, UNUSED, pooled).astype(BF16)
    for i in range(pay_ref.shape[0]):
        pay_ref[i] = payload


def project_blocks(got_ref, wq_ref, wk_ref, wv_ref):
    weight = jnp.concatenate([wq_ref[...], wk_ref[...], wv_ref[...]], axis=1)
    here, rows = [], []
    for k in range(got_ref.shape[0] // 4):
        parts = [got_ref[4 * k + t].astype(F32) for t in range(4)]
        used = (parts[0][:, 0:1] < 0.1 * UNUSED).astype(F32)
        here.append(jnp.sum(used, axis=0, keepdims=True))
        square = sum(jnp.sum(p * p, axis=-1, keepdims=True) for p in parts)
        scale = used * lax.rsqrt(square * (1.0 / DB) + EPSILON)
        rows.append(jnp.concatenate([(p * scale).astype(BF16) for p in parts], axis=1))
    return here, dot(jnp.concatenate(rows, axis=0), weight).astype(BF16)


def own_latent_kernel(own_ref, wq_ref, wk_ref, wv_ref, made_ref, count_ref):
    here, made = project_blocks(own_ref, wq_ref, wk_ref, wv_ref)
    made_ref[...] = made
    for k, filled in enumerate(here):
        count_ref[k : k + 1] = jnp.broadcast_to(filled, (1, count_ref.shape[1]))


def latent_kernel(core_ref, made_ref, count_ref, other_ref, wq_ref, wk_ref, wv_ref, q_ref, kv_ref, place_ref):
    blocks = other_ref.shape[0] // 4
    slots = 2 * blocks * ROWS
    is_odd = (core_ref[0] > 0).astype(F32)
    here, made = project_blocks(other_ref, wq_ref, wk_ref, wv_ref)
    here = [count_ref[k : k + 1, 0:1] for k in range(blocks)] + here
    made = jnp.concatenate([made_ref[...], made], axis=0)
    slot = iota((1, slots), 1)
    place = jnp.full((1, slots), -1.0, F32)
    total = jnp.zeros((1, 1), F32)
    for c in range(blocks):
        own, other = here[c], here[blocks + c]
        for k, filled, ahead in ((c, own, total + other * is_odd), (blocks + c, other, total + own * (1.0 - is_odd))):
            order = (slot - ROWS * k).astype(F32)
            place = jnp.where((order >= 0.0) & (order < filled), order + ahead, place)
        total = total + own + other
    place = place.astype(jnp.int32)
    place_ref[...] = jnp.broadcast_to(place, place_ref.shape)
    pick = (iota((GROUP, slots), 0) == place).astype(F32).astype(BF16)
    packed = dot(pick, made)
    q_ref[...] = packed[:, 0:HEAD_L].astype(BF16)
    kv_ref[0:GROUP, 0:HEAD_L] = packed[:, HEAD_L : 2 * HEAD_L].astype(BF16)
    value = packed[:, 2 * HEAD_L :]
    largest = jnp.max(jnp.max(jnp.abs(value), axis=1, keepdims=True), axis=0, keepdims=True)
    power = jnp.clip(13.0 - jnp.ceil(jnp.log2(jnp.maximum(largest, 1e-35))), -20.0, 100.0)
    kv_ref[0:GROUP, HEAD_L:] = (value * jnp.exp2(power)).astype(BF16)
    high = total.astype(BF16).astype(F32)
    row = iota((KVROWS - GROUP, 2 * HEAD_L), 0)
    tail = jnp.where(row == 0, high, jnp.where(row == 1, total - high, jnp.where(row == 2, power, 0.0)))
    kv_ref[GROUP:, :] = tail.astype(BF16)


SCALE = 1.0 / (math.sqrt(HEAD_L) * math.log(2.0))


def attend_kernel(z_ref, q_ref, kv_ref, place_ref, w_hbm, out_ref, theirs_ref, m_ref, l_ref, acc_ref, w_ref, sem):
    load = pltpu.make_async_copy(w_hbm, w_ref, sem)
    load.start()
    m_ref[...] = jnp.full(m_ref.shape, NEGATIVE, F32)
    l_ref[...] = jnp.zeros(l_ref.shape, F32)
    acc_ref[...] = jnp.zeros(acc_ref.shape, F32)
    z = z_ref[0]
    count = kv_ref.shape[0]
    spans, done = [], 0
    for span in SPANS + (4,) * count:
        if done < count:
            spans.append((done, min(done + span, count)))
            done += span
    for begin, end in spans:

        @pl.when(z >= begin)
        def _(begin=begin, end=end):
            codes, scores = [], []
            for b in range(begin, end):
                filled = kv_ref[b, GROUP : GROUP + 1, 0:1].astype(F32) + kv_ref[b, GROUP + 1 : GROUP + 2, 0:1].astype(F32)
                spot = iota((1, GROUP), 1)
                past = jnp.where(spot.astype(F32) < filled, -1, GROUP)
                codes.append(jnp.where(z > b, past, jnp.where(z == b, spot, GROUP)))
                scores.append(dot_nt(q_ref[...], kv_ref[b, 0:GROUP, 0:HEAD_L]))
            code = jnp.concatenate(codes, axis=1)
            score = jnp.concatenate(scores, axis=1) * SCALE
            score = jnp.where(code <= iota((GROUP, 1), 0), score, NEGATIVE)
            old = m_ref[:, 0:1]
            highest = jnp.maximum(old, jnp.max(score, axis=-1, keepdims=True))
            factor = jnp.exp2(old - highest)
            weights = jnp.exp2(score - highest)
            m_ref[...] = jnp.broadcast_to(highest, m_ref.shape)
            l_ref[...] = l_ref[...] * factor + jnp.sum(weights, axis=-1, keepdims=True)
            weights = weights.astype(BF16)
            mixed = acc_ref[...] * factor
            for k, b in enumerate(range(begin, end)):
                back = jnp.exp2(-kv_ref[b, GROUP + 2 : GROUP + 3, 0:1].astype(F32))
                mixed = mixed + dot(weights[:, GROUP * k : GROUP * (k + 1)], kv_ref[b, 0:GROUP, HEAD_L:]) * back
            acc_ref[...] = mixed

    mixed = (acc_ref[...] / l_ref[...]).astype(BF16)
    out_ref[...] = mixed
    load.wait()
    write_shares(mixed, place_ref, w_ref, theirs_ref, 1)


def write_shares(mixed, place_ref, w_ref, shares_ref, half):
    slots = place_ref.shape[1] // 2
    place = place_ref[0:1][:, slots * half : slots * (half + 1)]
    pick = (iota((GROUP, slots), 0) == place).astype(F32).astype(BF16)
    spread = dot_tn(pick, mixed).astype(BF16)
    width = shares_ref.shape[2]
    for t in range(4):
        part = dot(spread, w_ref[:, width * t : width * (t + 1)]).astype(BF16)
        for c in range(slots // ROWS):
            shares_ref[4 * c + t] = part[ROWS * c : ROWS * (c + 1)]


def share_kernel(mixed_ref, place_ref, w_ref, mine_ref):
    write_shares(mixed_ref[...], place_ref, w_ref, mine_ref, 0)


def output_kernel(got_ref, enc_ref, member_ref, out_ref):
    decoded = got_ref[0].astype(F32)
    for h in range(1, got_ref.shape[0]):
        decoded = decoded + got_ref[h].astype(F32)
    high = decoded.astype(BF16)
    low = (decoded - high.astype(F32)).astype(BF16)
    members = member_ref[...]
    out_ref[...] = (enc_ref[...].astype(F32) + dot_tn(members, high) + dot_tn(members, low)).astype(BF16)


def call(kernel, shapes, specs, *args, scratch=(), grant=16):
    single = not isinstance(shapes, list)
    structs = [jax.ShapeDtypeStruct(s, d) for s, d in ([shapes] if single else shapes)]
    return pl.pallas_call(
        kernel,
        out_shape=structs[0] if single else structs,
        in_specs=specs,
        out_specs=VMEM if single else [VMEM] * len(structs),
        scratch_shapes=scratch,
        compiler_params=pltpu.CompilerParams(vmem_limit_bytes=grant << 20),
    )(*args)


def scalar(value):
    return value.astype(jnp.int32).reshape(1)


def swap_cores(value):
    return lax.ppermute(value, "core", [(0, 1), (1, 0)])


def exchange(value):
    return lax.all_to_all(value, ("x", "tp"), split_axis=0, concat_axis=0, tiled=True)


def gather_keys(kv):
    size = lax.axis_size("bytes")
    got = lax.all_gather(kv.astype(jnp.float16), "bytes", axis=0, tiled=True)
    return got.astype(BF16).reshape(size, *kv.shape)


def per_device(ids, offsets, byte_table, byte_query, byte_key, byte_value, latent_query, latent_key, latent_value, decode_weight):
    n = ids.shape[0]
    width = byte_query.shape[1]
    ring = ("bytes", "x", "core")
    plane = lax.axis_size(("x", "tp"))
    earlier = lax.ppermute(ids, ring, [(i, i + 1) for i in range(lax.axis_size(ring) - 1)])
    weights = [pltpu.with_memory_space_constraint(w, pltpu.HBM) for w in (byte_table, byte_query, byte_key, byte_value)]
    table = call(
        table_kernel,
        ((byte_table.shape[0], 3 * width), BF16),
        [pl.BlockSpec(memory_space=pltpu.HBM)] * 4,
        *weights,
        scratch=[pltpu.VMEM(w.shape, BF16) for w in weights] + [pltpu.SemaphoreType.DMA((4, PIECES))],
    )
    part = call(
        own_byte_kernel,
        [((n, width), BF16), ((n, width), F32), ((n, HEAD_L), F32), ((ROWS, n), BF16)],
        [VMEM] * 3,
        ids.reshape(1, n), offsets.reshape(1, n), table,
    )
    members = part[3]
    encoded, payload = call(
        byte_kernel,
        [((n, width), BF16), ((plane, ROWS, width), BF16)],
        [SMEM] + [VMEM] * 6,
        scalar(lax.axis_index(ring)), earlier.reshape(1, n), table, *part,
    )
    own = exchange(payload)
    other = swap_cores(own)
    projections = (latent_query, latent_key, latent_value)
    half = ROWS * plane // 4
    made, counts = call(
        own_latent_kernel, [((half, 3 * HEAD_L), BF16), ((8, HEAD_L), F32)], [VMEM] * 4, own, *projections
    )
    queries, kv, place = call(
        latent_kernel,
        [((GROUP, HEAD_L), BF16), ((KVROWS, 2 * HEAD_L), BF16), ((8, 2 * half), jnp.int32)],
        [SMEM] + [VMEM] * 6,
        scalar(lax.axis_index("core")), made, counts, other, *projections,
    )
    shape = ((plane, SLOTS, width), BF16)
    decode = pltpu.with_memory_space_constraint(decode_weight, pltpu.HBM)
    mixed, theirs = call(
        attend_kernel,
        [((GROUP, HEAD_L), BF16), shape],
        [SMEM] + [VMEM] * 3 + [pl.BlockSpec(memory_space=pltpu.HBM)],
        scalar(lax.axis_index("bytes")), queries, gather_keys(kv), place, decode,
        scratch=[pltpu.VMEM((GROUP, HEAD_L), F32)] * 3
        + [pltpu.VMEM(decode_weight.shape, BF16), pltpu.SemaphoreType.DMA(())],
        grant=32,
    )
    mine = call(share_kernel, shape, [VMEM] * 3, mixed, place, decode)
    shares = (mine.astype(F32) + swap_cores(theirs).astype(F32)).astype(BF16)
    return call(output_kernel, ((n, width), BF16), [VMEM] * 3, exchange(shares), encoded, members)


def solution(mesh):
    sizes = mesh.shape
    finer = jax.sharding.Mesh(
        mesh.devices.reshape(sizes["bytes"], sizes["ctx"] // 2, 2, sizes["tp"]), ("bytes", "x", "core", "tp")
    )
    rows, heads = ("bytes", "x", "core"), ("x", "core", "tp")
    return jax.shard_map(
        per_device,
        mesh=finer,
        in_specs=(
            P(rows),
            P(rows),
            P(),
            P(None, "tp"),
            P(None, "tp"),
            P(None, "tp"),
            P(None, heads),
            P(None, heads),
            P(None, heads),
            P(heads, None),
        ),
        out_specs=P(rows, "tp"),
        check_vma=False,
    )
```

```python
import math

import jax
import jax.numpy as jnp
from jax import lax
from jax.experimental import pallas as pl
from jax.experimental.pallas import tpu as pltpu
from jax.sharding import PartitionSpec as P

DB = 1024
HEADS_B = 16
HEAD_L = 128
SLOTS = 72
ROWS = 72
UNUSED = 1e9
GROUP = 384
KVROWS = 392
SPANS = (1, 3, 4, 4, 4)
EPSILON = 1e-06
NEGATIVE = -1e30
F32 = jnp.float32
BF16 = jnp.bfloat16

VMEM = pl.BlockSpec(memory_space=pltpu.VMEM)
SMEM = pl.BlockSpec(memory_space=pltpu.SMEM)


def iota(shape, dim):
    return lax.broadcasted_iota(jnp.int32, shape, dim)


def dot(a, b):
    return jnp.dot(a, b, preferred_element_type=F32)


def dot_nt(a, b):
    return lax.dot_general(a, b, (((1,), (1,)), ((), ())), preferred_element_type=F32)


def dot_tn(a, b):
    return lax.dot_general(a, b, (((0,), (0,)), ((), ())), preferred_element_type=F32)


PIECES = 4


def table_kernel(table_hbm, wq_hbm, wk_hbm, wv_hbm, out_ref, table_ref, wq_ref, wk_ref, wv_ref, sems):
    pairs = ((table_hbm, table_ref), (wq_hbm, wq_ref), (wk_hbm, wk_ref), (wv_hbm, wv_ref))
    copies = []
    for k, (source, target) in enumerate(pairs):
        rows = source.shape[0] // PIECES
        part = [pl.ds(rows * i, rows) for i in range(PIECES)]
        copies.append([pltpu.make_async_copy(source.at[p], target.at[p], sems.at[k, i]) for i, p in enumerate(part)])
        for copy in copies[-1]:
            copy.start()
    for copy in copies[0]:
        copy.wait()
    embedded = table_ref[...].astype(F32)
    scale = lax.rsqrt(jnp.mean(embedded * embedded, axis=-1, keepdims=True) + EPSILON)
    normed = (embedded * scale).astype(BF16)
    width = wq_ref.shape[1]
    for k, w_ref in enumerate((wq_ref, wk_ref, wv_ref)):
        for copy in copies[k + 1]:
            copy.wait()
        out_ref[:, width * k : width * (k + 1)] = dot(normed, w_ref[...]).astype(BF16)


HEAD_B = 64


def head_column(width, h):
    column = iota((1, width), 1)
    return ((column >= h * HEAD_B) & (column < (h + 1) * HEAD_B)).astype(F32).astype(BF16)


def own_byte_kernel(ids_ref, offsets_ref, table_ref, own_ref, member_ref):
    n = ids_ref.shape[1]
    onehot = (iota((table_ref.shape[0], n), 0) == ids_ref[...]).astype(F32).astype(BF16)
    own_ref[...] = dot_tn(onehot, table_ref[...]).astype(BF16)
    starts = (offsets_ref[...] == 0).astype(F32)
    upto = (iota((n, n), 0) <= iota((n, n), 1)).astype(F32).astype(BF16)
    running = dot(jnp.broadcast_to(starts, (8, n)).astype(BF16), upto)[0:1]
    patch = running.astype(jnp.int32) - 1
    member_ref[...] = (iota((ROWS, n), 0) == patch).astype(F32).astype(BF16)


def byte_kernel(block_ref, earlier_ref, table_ref, own_ref, member_ref, enc_ref, pay_ref):
    n, width = enc_ref.shape
    onehot = (iota((table_ref.shape[0], n), 0) == earlier_ref[...]).astype(F32).astype(BF16)
    before = dot_tn(onehot, table_ref[:, width:]).astype(BF16)
    own = own_ref[...]
    queries = own[:, :width]
    keys = jnp.concatenate([before[:, :width], own[:, width : 2 * width]], axis=0)
    values = jnp.concatenate([before[:, width:], own[:, 2 * width :]], axis=0)
    query_pos = iota((n, 2 * n), 0)
    key_pos = iota((n, 2 * n), 1)
    first = jnp.where(block_ref[0] > 0, 0, n)
    allowed = (key_pos > query_pos) & (key_pos <= query_pos + n) & (key_pos >= first)
    encoded = jnp.zeros((n, width), F32)
    for h in range(width // HEAD_B):
        mine = head_column(width, h)
        scores = dot_nt(queries * mine, keys) * (1.0 / math.sqrt(HEAD_B))
        scores = jnp.where(allowed, scores, NEGATIVE)
        weights = jnp.exp(scores - jnp.max(scores, axis=-1, keepdims=True))
        totals = jnp.sum(weights, axis=-1, keepdims=True)
        encoded = encoded + dot(weights.astype(BF16), values * mine) / totals
    encoded = encoded.astype(BF16)
    enc_ref[...] = encoded
    members = member_ref[...]
    lengths = jnp.sum(members.astype(F32), axis=1, keepdims=True)
    pooled = dot(members, encoded) / jnp.maximum(lengths, 1.0)
    empty = (lengths < 0.5) & (iota((ROWS, width), 1) == 0)
    payload = jnp.where(empty, UNUSED, pooled).astype(BF16)
    for i in range(pay_ref.shape[0]):
        pay_ref[i] = payload


def project_blocks(got_ref, wq_ref, wk_ref, wv_ref):
    weight = jnp.concatenate([wq_ref[...], wk_ref[...], wv_ref[...]], axis=1)
    here, rows = [], []
    for k in range(got_ref.shape[0] // 4):
        parts = [got_ref[4 * k + t].astype(F32) for t in range(4)]
        used = (parts[0][:, 0:1] < 0.1 * UNUSED).astype(F32)
        here.append(jnp.sum(used, axis=0, keepdims=True))
        square = sum(jnp.sum(p * p, axis=-1, keepdims=True) for p in parts)
        scale = used * lax.rsqrt(square * (1.0 / DB) + EPSILON)
        rows.append(jnp.concatenate([(p * scale).astype(BF16) for p in parts], axis=1))
    return here, dot(jnp.concatenate(rows, axis=0), weight).astype(BF16)


def own_latent_kernel(own_ref, wq_ref, wk_ref, wv_ref, made_ref, count_ref):
    here, made = project_blocks(own_ref, wq_ref, wk_ref, wv_ref)
    made_ref[...] = made
    for k, filled in enumerate(here):
        count_ref[k : k + 1] = jnp.broadcast_to(filled, (1, count_ref.shape[1]))


def latent_kernel(core_ref, made_ref, count_ref, other_ref, wq_ref, wk_ref, wv_ref, q_ref, kv_ref, place_ref):
    blocks = other_ref.shape[0] // 4
    slots = 2 * blocks * ROWS
    is_odd = (core_ref[0] > 0).astype(F32)
    here, made = project_blocks(other_ref, wq_ref, wk_ref, wv_ref)
    here = [count_ref[k : k + 1, 0:1] for k in range(blocks)] + here
    made = jnp.concatenate([made_ref[...], made], axis=0)
    slot = iota((1, slots), 1)
    place = jnp.full((1, slots), -1.0, F32)
    total = jnp.zeros((1, 1), F32)
    for c in range(blocks):
        own, other = here[c], here[blocks + c]
        for k, filled, ahead in ((c, own, total + other * is_odd), (blocks + c, other, total + own * (1.0 - is_odd))):
            order = (slot - ROWS * k).astype(F32)
            place = jnp.where((order >= 0.0) & (order < filled), order + ahead, place)
        total = total + own + other
    place = place.astype(jnp.int32)
    place_ref[...] = jnp.broadcast_to(place, place_ref.shape)
    pick = (iota((GROUP, slots), 0) == place).astype(F32).astype(BF16)
    packed = dot(pick, made)
    q_ref[...] = packed[:, 0:HEAD_L].astype(BF16)
    kv_ref[0:GROUP, 0:HEAD_L] = packed[:, HEAD_L : 2 * HEAD_L].astype(BF16)
    value = packed[:, 2 * HEAD_L :]
    largest = jnp.max(jnp.max(jnp.abs(value), axis=1, keepdims=True), axis=0, keepdims=True)
    power = jnp.clip(13.0 - jnp.ceil(jnp.log2(jnp.maximum(largest, 1e-35))), -20.0, 100.0)
    kv_ref[0:GROUP, HEAD_L:] = (value * jnp.exp2(power)).astype(BF16)
    high = total.astype(BF16).astype(F32)
    row = iota((KVROWS - GROUP, 2 * HEAD_L), 0)
    tail = jnp.where(row == 0, high, jnp.where(row == 1, total - high, jnp.where(row == 2, power, 0.0)))
    kv_ref[GROUP:, :] = tail.astype(BF16)


SCALE = 1.0 / (math.sqrt(HEAD_L) * math.log(2.0))


def attend_kernel(z_ref, q_ref, kv_ref, place_ref, w_hbm, out_ref, theirs_ref, m_ref, l_ref, acc_ref, w_ref, sem):
    load = pltpu.make_async_copy(w_hbm, w_ref, sem)
    load.start()
    m_ref[...] = jnp.full(m_ref.shape, NEGATIVE, F32)
    l_ref[...] = jnp.zeros(l_ref.shape, F32)
    acc_ref[...] = jnp.zeros(acc_ref.shape, F32)
    z = z_ref[0]
    count = kv_ref.shape[0]
    spans, done = [], 0
    for span in SPANS + (4,) * count:
        if done < count:
            spans.append((done, min(done + span, count)))
            done += span
    for begin, end in spans:

        @pl.when(z >= begin)
        def _(begin=begin, end=end):
            codes, scores = [], []
            for b in range(begin, end):
                filled = kv_ref[b, GROUP : GROUP + 1, 0:1].astype(F32) + kv_ref[b, GROUP + 1 : GROUP + 2, 0:1].astype(F32)
                spot = iota((1, GROUP), 1)
                past = jnp.where(spot.astype(F32) < filled, -1, GROUP)
                codes.append(jnp.where(z > b, past, jnp.where(z == b, spot, GROUP)))
                scores.append(dot_nt(q_ref[...], kv_ref[b, 0:GROUP, 0:HEAD_L]))
            code = jnp.concatenate(codes, axis=1)
            score = jnp.concatenate(scores, axis=1) * SCALE
            score = jnp.where(code <= iota((GROUP, 1), 0), score, NEGATIVE)
            old = m_ref[:, 0:1]
            highest = jnp.maximum(old, jnp.max(score, axis=-1, keepdims=True))
            factor = jnp.exp2(old - highest)
            weights = jnp.exp2(score - highest)
            m_ref[...] = jnp.broadcast_to(highest, m_ref.shape)
            l_ref[...] = l_ref[...] * factor + jnp.sum(weights, axis=-1, keepdims=True)
            weights = weights.astype(BF16)
            mixed = acc_ref[...] * factor
            for k, b in enumerate(range(begin, end)):
                back = jnp.exp2(-kv_ref[b, GROUP + 2 : GROUP + 3, 0:1].astype(F32))
                mixed = mixed + dot(weights[:, GROUP * k : GROUP * (k + 1)], kv_ref[b, 0:GROUP, HEAD_L:]) * back
            acc_ref[...] = mixed

    mixed = (acc_ref[...] / l_ref[...]).astype(BF16)
    out_ref[...] = mixed
    load.wait()
    write_shares(mixed, place_ref, w_ref, theirs_ref, 1)


def write_shares(mixed, place_ref, w_ref, shares_ref, half):
    slots = place_ref.shape[1] // 2
    place = place_ref[0:1][:, slots * half : slots * (half + 1)]
    pick = (iota((GROUP, slots), 0) == place).astype(F32).astype(BF16)
    spread = dot_tn(pick, mixed).astype(BF16)
    width = shares_ref.shape[2]
    for t in range(4):
        part = dot(spread, w_ref[:, width * t : width * (t + 1)]).astype(BF16)
        for c in range(slots // ROWS):
            shares_ref[4 * c + t] = part[ROWS * c : ROWS * (c + 1)]


def share_kernel(mixed_ref, place_ref, w_ref, mine_ref):
    write_shares(mixed_ref[...], place_ref, w_ref, mine_ref, 0)


def output_kernel(got_ref, enc_ref, member_ref, out_ref):
    decoded = got_ref[0].astype(F32)
    for h in range(1, got_ref.shape[0]):
        decoded = decoded + got_ref[h].astype(F32)
    high = decoded.astype(BF16)
    low = (decoded - high.astype(F32)).astype(BF16)
    members = member_ref[...]
    out_ref[...] = (enc_ref[...].astype(F32) + dot_tn(members, high) + dot_tn(members, low)).astype(BF16)


def call(kernel, shapes, specs, *args, scratch=(), grant=16):
    single = not isinstance(shapes, list)
    structs = [jax.ShapeDtypeStruct(s, d) for s, d in ([shapes] if single else shapes)]
    return pl.pallas_call(
        kernel,
        out_shape=structs[0] if single else structs,
        in_specs=specs,
        out_specs=VMEM if single else [VMEM] * len(structs),
        scratch_shapes=scratch,
        compiler_params=pltpu.CompilerParams(vmem_limit_bytes=grant << 20),
    )(*args)


def scalar(value):
    return value.astype(jnp.int32).reshape(1)


def swap_cores(value):
    return lax.ppermute(value, "core", [(0, 1), (1, 0)])


def exchange(value):
    return lax.all_to_all(value, ("x", "tp"), split_axis=0, concat_axis=0, tiled=True)


def gather_keys(kv):
    size = lax.axis_size("bytes")
    got = lax.all_gather(kv.astype(jnp.float16), "bytes", axis=0, tiled=True)
    return got.astype(BF16).reshape(size, *kv.shape)


def per_device(ids, offsets, byte_table, byte_query, byte_key, byte_value, latent_query, latent_key, latent_value, decode_weight):
    n = ids.shape[0]
    width = byte_query.shape[1]
    ring = ("bytes", "x", "core")
    plane = lax.axis_size(("x", "tp"))
    earlier = lax.ppermute(ids, ring, [(i, i + 1) for i in range(lax.axis_size(ring) - 1)])
    weights = [pltpu.with_memory_space_constraint(w, pltpu.HBM) for w in (byte_table, byte_query, byte_key, byte_value)]
    table = call(
        table_kernel,
        ((byte_table.shape[0], 3 * width), BF16),
        [pl.BlockSpec(memory_space=pltpu.HBM)] * 4,
        *weights,
        scratch=[pltpu.VMEM(w.shape, BF16) for w in weights] + [pltpu.SemaphoreType.DMA((4, PIECES))],
    )
    looked_up, members = call(
        own_byte_kernel,
        [((n, 3 * width), BF16), ((ROWS, n), BF16)],
        [VMEM] * 3,
        ids.reshape(1, n), offsets.reshape(1, n), table,
    )
    encoded, payload = call(
        byte_kernel,
        [((n, width), BF16), ((plane, ROWS, width), BF16)],
        [SMEM] + [VMEM] * 4,
        scalar(lax.axis_index(ring)), earlier.reshape(1, n), table, looked_up, members,
    )
    own = exchange(payload)
    other = swap_cores(own)
    projections = (latent_query, latent_key, latent_value)
    half = ROWS * plane // 4
    made, counts = call(
        own_latent_kernel, [((half, 3 * HEAD_L), BF16), ((8, HEAD_L), F32)], [VMEM] * 4, own, *projections
    )
    queries, kv, place = call(
        latent_kernel,
        [((GROUP, HEAD_L), BF16), ((KVROWS, 2 * HEAD_L), BF16), ((8, 2 * half), jnp.int32)],
        [SMEM] + [VMEM] * 6,
        scalar(lax.axis_index("core")), made, counts, other, *projections,
    )
    shape = ((plane, SLOTS, width), BF16)
    decode = pltpu.with_memory_space_constraint(decode_weight, pltpu.HBM)
    mixed, theirs = call(
        attend_kernel,
        [((GROUP, HEAD_L), BF16), shape],
        [SMEM] + [VMEM] * 3 + [pl.BlockSpec(memory_space=pltpu.HBM)],
        scalar(lax.axis_index("bytes")), queries, gather_keys(kv), place, decode,
        scratch=[pltpu.VMEM((GROUP, HEAD_L), F32)] * 3
        + [pltpu.VMEM(decode_weight.shape, BF16), pltpu.SemaphoreType.DMA(())],
        grant=32,
    )
    mine = call(share_kernel, shape, [VMEM] * 3, mixed, place, decode)
    shares = (mine.astype(F32) + swap_cores(theirs).astype(F32)).astype(BF16)
    return call(output_kernel, ((n, width), BF16), [VMEM] * 3, exchange(shares), encoded, members)


def solution(mesh):
    sizes = mesh.shape
    finer = jax.sharding.Mesh(
        mesh.devices.reshape(sizes["bytes"], sizes["ctx"] // 2, 2, sizes["tp"]), ("bytes", "x", "core", "tp")
    )
    rows, heads = ("bytes", "x", "core"), ("x", "core", "tp")
    return jax.shard_map(
        per_device,
        mesh=finer,
        in_specs=(
            P(rows),
            P(rows),
            P(),
            P(None, "tp"),
            P(None, "tp"),
            P(None, "tp"),
            P(None, heads),
            P(None, heads),
            P(None, heads),
            P(heads, None),
        ),
        out_specs=P(rows, "tp"),
        check_vma=False,
    )
```

```python
import math

import jax
import jax.numpy as jnp
from jax import lax
from jax.experimental import pallas as pl
from jax.experimental.pallas import tpu as pltpu
from jax.sharding import PartitionSpec as P

DB = 1024
HEADS_B = 16
HEAD_L = 128
SLOTS = 72
ROWS = 72
UNUSED = 1e9
GROUP = 384
KVROWS = 392
SPANS = (1, 2, 4, 4, 5)
EPSILON = 1e-06
NEGATIVE = -1e30
F32 = jnp.float32
BF16 = jnp.bfloat16

VMEM = pl.BlockSpec(memory_space=pltpu.VMEM)
SMEM = pl.BlockSpec(memory_space=pltpu.SMEM)


def iota(shape, dim):
    return lax.broadcasted_iota(jnp.int32, shape, dim)


def dot(a, b):
    return jnp.dot(a, b, preferred_element_type=F32)


def dot_nt(a, b):
    return lax.dot_general(a, b, (((1,), (1,)), ((), ())), preferred_element_type=F32)


def dot_tn(a, b):
    return lax.dot_general(a, b, (((0,), (0,)), ((), ())), preferred_element_type=F32)


PIECES = 4


def table_kernel(table_hbm, wq_hbm, wk_hbm, wv_hbm, out_ref, table_ref, wq_ref, wk_ref, wv_ref, sems):
    pairs = ((table_hbm, table_ref), (wq_hbm, wq_ref), (wk_hbm, wk_ref), (wv_hbm, wv_ref))
    copies = []
    for k, (source, target) in enumerate(pairs):
        rows = source.shape[0] // PIECES
        part = [pl.ds(rows * i, rows) for i in range(PIECES)]
        copies.append([pltpu.make_async_copy(source.at[p], target.at[p], sems.at[k, i]) for i, p in enumerate(part)])
        for copy in copies[-1]:
            copy.start()
    for copy in copies[0]:
        copy.wait()
    embedded = table_ref[...].astype(F32)
    scale = lax.rsqrt(jnp.mean(embedded * embedded, axis=-1, keepdims=True) + EPSILON)
    normed = (embedded * scale).astype(BF16)
    width = wq_ref.shape[1]
    for k, w_ref in enumerate((wq_ref, wk_ref, wv_ref)):
        for copy in copies[k + 1]:
            copy.wait()
        out_ref[:, width * k : width * (k + 1)] = dot(normed, w_ref[...]).astype(BF16)


HEAD_B = 64


def head_column(width, h):
    column = iota((1, width), 1)
    return ((column >= h * HEAD_B) & (column < (h + 1) * HEAD_B)).astype(F32).astype(BF16)


def own_byte_kernel(ids_ref, offsets_ref, table_ref, own_ref, member_ref):
    n = ids_ref.shape[1]
    onehot = (iota((table_ref.shape[0], n), 0) == ids_ref[...]).astype(F32).astype(BF16)
    own_ref[...] = dot_tn(onehot, table_ref[...]).astype(BF16)
    starts = (offsets_ref[...] == 0).astype(F32)
    upto = (iota((n, n), 0) <= iota((n, n), 1)).astype(F32).astype(BF16)
    running = dot(jnp.broadcast_to(starts, (8, n)).astype(BF16), upto)[0:1]
    patch = running.astype(jnp.int32) - 1
    member_ref[...] = (iota((ROWS, n), 0) == patch).astype(F32).astype(BF16)


def byte_kernel(block_ref, earlier_ref, table_ref, own_ref, member_ref, enc_ref, pay_ref):
    n, width = enc_ref.shape
    onehot = (iota((table_ref.shape[0], n), 0) == earlier_ref[...]).astype(F32).astype(BF16)
    before = dot_tn(onehot, table_ref[:, width:]).astype(BF16)
    own = own_ref[...]
    queries = own[:, :width]
    keys = jnp.concatenate([before[:, :width], own[:, width : 2 * width]], axis=0)
    values = jnp.concatenate([before[:, width:], own[:, 2 * width :]], axis=0)
    query_pos = iota((n, 2 * n), 0)
    key_pos = iota((n, 2 * n), 1)
    first = jnp.where(block_ref[0] > 0, 0, n)
    allowed = (key_pos > query_pos) & (key_pos <= query_pos + n) & (key_pos >= first)
    encoded = jnp.zeros((n, width), F32)
    for h in range(width // HEAD_B):
        mine = head_column(width, h)
        scores = dot_nt(queries * mine, keys) * (1.0 / math.sqrt(HEAD_B))
        scores = jnp.where(allowed, scores, NEGATIVE)
        weights = jnp.exp(scores - jnp.max(scores, axis=-1, keepdims=True))
        totals = jnp.sum(weights, axis=-1, keepdims=True)
        encoded = encoded + dot(weights.astype(BF16), values * mine) * (1.0 / totals)
    encoded = encoded.astype(BF16)
    enc_ref[...] = encoded
    members = member_ref[...]
    lengths = jnp.sum(members.astype(F32), axis=1, keepdims=True)
    pooled = dot(members, encoded) / jnp.maximum(lengths, 1.0)
    empty = (lengths < 0.5) & (iota((ROWS, width), 1) == 0)
    payload = jnp.where(empty, UNUSED, pooled).astype(BF16)
    for i in range(pay_ref.shape[0]):
        pay_ref[i] = payload


def project_blocks(got_ref, wq_ref, wk_ref, wv_ref):
    weight = jnp.concatenate([wq_ref[...], wk_ref[...], wv_ref[...]], axis=1)
    here, rows = [], []
    for k in range(got_ref.shape[0] // 4):
        parts = [got_ref[4 * k + t].astype(F32) for t in range(4)]
        used = (parts[0][:, 0:1] < 0.1 * UNUSED).astype(F32)
        here.append(jnp.sum(used, axis=0, keepdims=True))
        square = sum(jnp.sum(p * p, axis=-1, keepdims=True) for p in parts)
        scale = used * lax.rsqrt(square * (1.0 / DB) + EPSILON)
        rows.append(jnp.concatenate([(p * scale).astype(BF16) for p in parts], axis=1))
    return here, dot(jnp.concatenate(rows, axis=0), weight).astype(BF16)


def own_latent_kernel(own_ref, wq_ref, wk_ref, wv_ref, made_ref, count_ref):
    here, made = project_blocks(own_ref, wq_ref, wk_ref, wv_ref)
    made_ref[...] = made
    for k, filled in enumerate(here):
        count_ref[k : k + 1] = jnp.broadcast_to(filled, (1, count_ref.shape[1]))


def latent_kernel(core_ref, made_ref, count_ref, other_ref, wq_ref, wk_ref, wv_ref, q_ref, kv_ref, place_ref):
    blocks = other_ref.shape[0] // 4
    slots = 2 * blocks * ROWS
    is_odd = (core_ref[0] > 0).astype(F32)
    here, made = project_blocks(other_ref, wq_ref, wk_ref, wv_ref)
    here = [count_ref[k : k + 1, 0:1] for k in range(blocks)] + here
    made = jnp.concatenate([made_ref[...], made], axis=0)
    slot = iota((1, slots), 1)
    place = jnp.full((1, slots), -1.0, F32)
    total = jnp.zeros((1, 1), F32)
    for c in range(blocks):
        own, other = here[c], here[blocks + c]
        for k, filled, ahead in ((c, own, total + other * is_odd), (blocks + c, other, total + own * (1.0 - is_odd))):
            order = (slot - ROWS * k).astype(F32)
            place = jnp.where((order >= 0.0) & (order < filled), order + ahead, place)
        total = total + own + other
    place = place.astype(jnp.int32)
    place_ref[...] = jnp.broadcast_to(place, place_ref.shape)
    pick = (iota((GROUP, slots), 0) == place).astype(F32).astype(BF16)
    packed = dot(pick, made)
    q_ref[...] = packed[:, 0:HEAD_L].astype(BF16)
    kv_ref[0:GROUP, 0:HEAD_L] = packed[:, HEAD_L : 2 * HEAD_L].astype(BF16)
    value = packed[:, 2 * HEAD_L :]
    largest = jnp.max(jnp.max(jnp.abs(value), axis=1, keepdims=True), axis=0, keepdims=True)
    power = jnp.clip(13.0 - jnp.ceil(jnp.log2(jnp.maximum(largest, 1e-35))), -20.0, 100.0)
    kv_ref[0:GROUP, HEAD_L:] = (value * jnp.exp2(power)).astype(BF16)
    high = total.astype(BF16).astype(F32)
    row = iota((KVROWS - GROUP, 2 * HEAD_L), 0)
    tail = jnp.where(row == 0, high, jnp.where(row == 1, total - high, jnp.where(row == 2, power, 0.0)))
    kv_ref[GROUP:, :] = tail.astype(BF16)


SCALE = 1.0 / (math.sqrt(HEAD_L) * math.log(2.0))


def attend_kernel(z_ref, q_ref, kv_ref, place_ref, w_hbm, out_ref, theirs_ref, m_ref, l_ref, acc_ref, w_ref, sem):
    load = pltpu.make_async_copy(w_hbm, w_ref, sem)
    load.start()
    m_ref[...] = jnp.full(m_ref.shape, NEGATIVE, F32)
    l_ref[...] = jnp.zeros(l_ref.shape, F32)
    acc_ref[...] = jnp.zeros(acc_ref.shape, F32)
    z = z_ref[0]
    count = kv_ref.shape[0]
    spans, done = [], 0
    for span in SPANS + (4,) * count:
        if done < count:
            spans.append((done, min(done + span, count)))
            done += span
    for begin, end in spans:

        @pl.when(z >= begin)
        def _(begin=begin, end=end):
            codes, scores = [], []
            for b in range(begin, end):
                filled = kv_ref[b, GROUP : GROUP + 1, 0:1].astype(F32) + kv_ref[b, GROUP + 1 : GROUP + 2, 0:1].astype(F32)
                spot = iota((1, GROUP), 1)
                past = jnp.where(spot.astype(F32) < filled, -1, GROUP)
                codes.append(jnp.where(z > b, past, jnp.where(z == b, spot, GROUP)))
                scores.append(dot_nt(q_ref[...], kv_ref[b, 0:GROUP, 0:HEAD_L]))
            code = jnp.concatenate(codes, axis=1)
            score = jnp.concatenate(scores, axis=1) * SCALE
            score = jnp.where(code <= iota((GROUP, 1), 0), score, NEGATIVE)
            old = m_ref[:, 0:1]
            highest = jnp.maximum(old, jnp.max(score, axis=-1, keepdims=True))
            factor = jnp.exp2(old - highest)
            weights = jnp.exp2(score - highest)
            m_ref[...] = jnp.broadcast_to(highest, m_ref.shape)
            l_ref[...] = l_ref[...] * factor + jnp.sum(weights, axis=-1, keepdims=True)
            weights = weights.astype(BF16)
            mixed = acc_ref[...] * factor
            for k, b in enumerate(range(begin, end)):
                back = jnp.exp2(-kv_ref[b, GROUP + 2 : GROUP + 3, 0:1].astype(F32))
                mixed = mixed + dot(weights[:, GROUP * k : GROUP * (k + 1)], kv_ref[b, 0:GROUP, HEAD_L:]) * back
            acc_ref[...] = mixed

    mixed = (acc_ref[...] / l_ref[...]).astype(BF16)
    out_ref[...] = mixed
    load.wait()
    write_shares(mixed, place_ref, w_ref, theirs_ref, 1)


def write_shares(mixed, place_ref, w_ref, shares_ref, half):
    slots = place_ref.shape[1] // 2
    place = place_ref[0:1][:, slots * half : slots * (half + 1)]
    pick = (iota((GROUP, slots), 0) == place).astype(F32).astype(BF16)
    spread = dot_tn(pick, mixed).astype(BF16)
    width = shares_ref.shape[2]
    for t in range(4):
        part = dot(spread, w_ref[:, width * t : width * (t + 1)]).astype(BF16)
        for c in range(slots // ROWS):
            shares_ref[4 * c + t] = part[ROWS * c : ROWS * (c + 1)]


def share_kernel(mixed_ref, place_ref, w_ref, mine_ref):
    write_shares(mixed_ref[...], place_ref, w_ref, mine_ref, 0)


def output_kernel(got_ref, enc_ref, member_ref, out_ref):
    decoded = got_ref[0].astype(F32)
    for h in range(1, got_ref.shape[0]):
        decoded = decoded + got_ref[h].astype(F32)
    high = decoded.astype(BF16)
    low = (decoded - high.astype(F32)).astype(BF16)
    members = jnp.concatenate([member_ref[...], member_ref[...]], axis=0)
    both = jnp.concatenate([high, low], axis=0)
    out_ref[...] = (enc_ref[...].astype(F32) + dot_tn(members, both)).astype(BF16)


def call(kernel, shapes, specs, *args, scratch=(), grant=16):
    single = not isinstance(shapes, list)
    structs = [jax.ShapeDtypeStruct(s, d) for s, d in ([shapes] if single else shapes)]
    return pl.pallas_call(
        kernel,
        out_shape=structs[0] if single else structs,
        in_specs=specs,
        out_specs=VMEM if single else [VMEM] * len(structs),
        scratch_shapes=scratch,
        compiler_params=pltpu.CompilerParams(vmem_limit_bytes=grant << 20),
    )(*args)


def scalar(value):
    return value.astype(jnp.int32).reshape(1)


def swap_cores(value):
    return lax.ppermute(value, "core", [(0, 1), (1, 0)])


def exchange(value):
    return lax.all_to_all(value, ("x", "tp"), split_axis=0, concat_axis=0, tiled=True)


def gather_keys(kv):
    size = lax.axis_size("bytes")
    got = lax.all_gather(kv.astype(jnp.float16), "bytes", axis=0, tiled=True)
    return got.astype(BF16).reshape(size, *kv.shape)


def per_device(ids, offsets, byte_table, byte_query, byte_key, byte_value, latent_query, latent_key, latent_value, decode_weight):
    n = ids.shape[0]
    width = byte_query.shape[1]
    ring = ("bytes", "x", "core")
    plane = lax.axis_size(("x", "tp"))
    earlier = lax.ppermute(ids, ring, [(i, i + 1) for i in range(lax.axis_size(ring) - 1)])
    weights = [pltpu.with_memory_space_constraint(w, pltpu.HBM) for w in (byte_table, byte_query, byte_key, byte_value)]
    table = call(
        table_kernel,
        ((byte_table.shape[0], 3 * width), BF16),
        [pl.BlockSpec(memory_space=pltpu.HBM)] * 4,
        *weights,
        scratch=[pltpu.VMEM(w.shape, BF16) for w in weights] + [pltpu.SemaphoreType.DMA((4, PIECES))],
    )
    looked_up, members = call(
        own_byte_kernel,
        [((n, 3 * width), BF16), ((ROWS, n), BF16)],
        [VMEM] * 3,
        ids.reshape(1, n), offsets.reshape(1, n), table,
    )
    encoded, payload = call(
        byte_kernel,
        [((n, width), BF16), ((plane, ROWS, width), BF16)],
        [SMEM] + [VMEM] * 4,
        scalar(lax.axis_index(ring)), earlier.reshape(1, n), table, looked_up, members,
    )
    own = exchange(payload)
    other = swap_cores(own)
    projections = (latent_query, latent_key, latent_value)
    half = ROWS * plane // 4
    made, counts = call(
        own_latent_kernel, [((half, 3 * HEAD_L), BF16), ((8, HEAD_L), F32)], [VMEM] * 4, own, *projections
    )
    queries, kv, place = call(
        latent_kernel,
        [((GROUP, HEAD_L), BF16), ((KVROWS, 2 * HEAD_L), BF16), ((8, 2 * half), jnp.int32)],
        [SMEM] + [VMEM] * 6,
        scalar(lax.axis_index("core")), made, counts, other, *projections,
    )
    shape = ((plane, SLOTS, width), BF16)
    decode = pltpu.with_memory_space_constraint(decode_weight, pltpu.HBM)
    mixed, theirs = call(
        attend_kernel,
        [((GROUP, HEAD_L), BF16), shape],
        [SMEM] + [VMEM] * 3 + [pl.BlockSpec(memory_space=pltpu.HBM)],
        scalar(lax.axis_index("bytes")), queries, gather_keys(kv), place, decode,
        scratch=[pltpu.VMEM((GROUP, HEAD_L), F32)] * 3
        + [pltpu.VMEM(decode_weight.shape, BF16), pltpu.SemaphoreType.DMA(())],
        grant=32,
    )
    mine = call(share_kernel, shape, [VMEM] * 3, mixed, place, decode)
    shares = (mine.astype(F32) + swap_cores(theirs).astype(F32)).astype(BF16)
    return call(output_kernel, ((n, width), BF16), [VMEM] * 3, exchange(shares), encoded, members)


def solution(mesh):
    sizes = mesh.shape
    finer = jax.sharding.Mesh(
        mesh.devices.reshape(sizes["bytes"], sizes["ctx"] // 2, 2, sizes["tp"]), ("bytes", "x", "core", "tp")
    )
    rows, heads = ("bytes", "x", "core"), ("x", "core", "tp")
    return jax.shard_map(
        per_device,
        mesh=finer,
        in_specs=(
            P(rows),
            P(rows),
            P(),
            P(None, "tp"),
            P(None, "tp"),
            P(None, "tp"),
            P(None, heads),
            P(None, heads),
            P(None, heads),
            P(heads, None),
        ),
        out_specs=P(rows, "tp"),
        check_vma=False,
    )
```
